512 devices in a mesh: row: 32 (over y, z_lo, core), col: 16 (over z_hi, x).
Axes of the slice: x: 4, y: 8, z: 8 (z_hi: 4, z_lo: 2; z = z_hi * 2 + z_lo), core: 2. Of those that a mesh axis runs over, the one named last changes fastest.
Arguments:
- residual: float32 [8192, 8192], P('row', 'col'), may hold values from -0.15625 to 0.15625
- direction: float32 [8192, 8192], P('row', 'col'), may hold values from -6 to 6
- ground_shift: float32 [1], replicated, may hold values from 1.6937256e-06 to 6.7749024e-06
- previous: float32 [1], replicated, may hold values from 3072 to 12288
Outputs:
- next_direction: float32 [8192, 8192], P('row', 'col')
- step_ratio: float32 [1], replicated
The draws below stay inside these ranges and needn't reach their ends.
All inputs are finite; a program needn't handle non-finite values.
Results may differ from the reference program's by a relative error of at most 0.00015.
Values sent between devices are 32-bit elements; how exact they have to be, the bound alone decides.
No kernel may reach another device: no remote copies, remote signals or barrier semaphores. Data moves between devices by JAX's collectives and lax.ppermute only.
A program may use at most 64 MiB of HBM per device.

```python
import math
import jax
import jax.numpy as jnp
from jax import lax

Q0 = 256
NX = 8192
NY = 8192


def draw_residual(key, part):
    subkeys = jax.random.split(jax.random.fold_in(key, 17), 2)
    row_place = jnp.arange(NX, dtype=jnp.int32).astype(jnp.float32) / NX
    col_scale = jnp.exp(jax.random.uniform(subkeys[1], (NY,), jnp.float32, 0.0, jnp.log(10.0)))
    base_scale = 0.1 / Q0
    row_scale = jnp.exp(row_place * jnp.log(10.0))
    samples = jnp.clip(jax.random.normal(subkeys[0], (NX, NY), jnp.float32), -4.0, 4.0)
    return base_scale * row_scale[:, None] * col_scale[None, :] * samples


def shard_levels(key, dims, cuts, low, largest):
    level = 1.0
    for axis_at, blocks in cuts:
        steps = jax.random.uniform(jax.random.fold_in(jax.random.fold_in(key, 6), axis_at), (blocks,), jnp.float32, low / len(cuts), largest / len(cuts))
        level = level * jnp.repeat(jnp.exp(steps), dims[axis_at] // blocks).reshape((-1,) + (1,) * (len(dims) - 1 - axis_at))
    return level


def gaussian(rng, dims, scale, reach, pieces=(), held_as=jnp.bfloat16):
    result = jax.random.normal(rng, dims, jnp.float32) * scale
    if len(pieces) > 0:
        result = shard_levels(rng, dims, pieces, -0.22, 0.18) * result
    return jnp.clip(result, min=-reach, max=reach).astype(held_as)


def setup_inputs(seed: int = 0) -> dict:
    streams_of = jax.random.split(jax.random.key(seed), 5)
    residual = draw_residual(jax.random.fold_in(streams_of[4], 71), 0)
    direction = gaussian(streams_of[1], (NX, NY), 1.0, 6.0, ((0, 32), (1, 16)), jnp.float32)
    ground_shift = jnp.clip(jnp.exp(jax.random.uniform(streams_of[2], (1,), jnp.float32, math.log(1.6937256077653728e-06), math.log(6.774902431061491e-06))), 1.6937256077653728e-06, 6.774902431061491e-06)
    previous = jnp.clip(jnp.exp(jax.random.uniform(streams_of[3], (1,), jnp.float32, math.log(3072.0), math.log(12288.0))), 3072.0, 12288.0)
    return dict(residual=residual, direction=direction, ground_shift=ground_shift, previous=previous)


PRECISE = lax.Precision.HIGHEST

def cosine_matrix(length):
    wavenum = jnp.arange(length, dtype=jnp.int32)[:, None]
    position = jnp.arange(length, dtype=jnp.int32)[None, :]
    phases = wavenum * (2 * position + 1) % (4 * length)
    angles = jnp.pi * phases.astype(jnp.float32) / (2 * length)
    scaling = jnp.where(wavenum == 0, jnp.sqrt(1.0 / length), jnp.sqrt(2.0 / length)).astype(jnp.float32)
    return scaling * jnp.cos(angles)

def reference(residual, direction, ground_shift, previous):
    rows_table = cosine_matrix(NX)
    cols_table = cosine_matrix(NY)
    spectrum = jnp.dot(jnp.dot(rows_table, residual, precision=PRECISE), cols_table.T, precision=PRECISE)
    row_waves = jnp.arange(NX, dtype=jnp.int32).astype(jnp.float32)
    col_waves = jnp.arange(NY, dtype=jnp.int32).astype(jnp.float32)
    row_sine = jnp.sin(jnp.pi * row_waves / (2 * NX))
    col_sine = jnp.sin(jnp.pi * col_waves / (2 * NY))
    eigenvalue = 4.0 * (row_sine * row_sine)[:, None] + 4.0 * (col_sine * col_sine)[None, :]
    weight = 1.0 / (eigenvalue + ground_shift[0])
    scaled = weight * spectrum
    precond = jnp.dot(jnp.dot(rows_table.T, scaled, precision=PRECISE), cols_table, precision=PRECISE)
    inner_total = jnp.sum(residual * precond)
    step_ratio = inner_total / previous[0]
    return (precond + step_ratio * direction, jnp.reshape(step_ratio, (1,)))
```

```python
import numpy as np
import jax
import jax.numpy as jnp
from jax import lax
from jax.sharding import PartitionSpec as P

ROW = "row"
COL = "col"
LANES = 128

HI = lax.Precision.HIGHEST


def mm(a, b, dims):
    return lax.dot_general(a, b, (dims, ((), ())), precision=HI)


def cosines(length):
    wave = np.arange(length)[:, None]
    place = np.arange(length)[None, :]
    angle = np.pi * (wave * (2 * place + 1) % (4 * length)) / (2 * length)
    scale = np.where(wave == 0, np.sqrt(1.0 / length), np.sqrt(2.0 / length))
    return scale * np.cos(angle)


def stiffness(waves, length):
    return 4.0 * np.sin(np.pi * waves / (2 * length)) ** 2


def sines(blocks):
    index = np.arange(blocks + 1)
    table = np.sqrt(2.0 / blocks) * np.sin(np.pi * (index[:, None] * index[None, :] % (2 * blocks)) / blocks)
    table[blocks] = 0.0
    return table[:, :blocks]


def block_constants(extent, blocks):
    table = cosines(extent)
    edge = table[:, 0]
    sign = np.where(np.arange(extent) % 2 == 0, 1.0, -1.0)
    dst = sines(blocks)
    theta = np.cos(np.pi * np.arange(blocks) / blocks)
    return dict(
        table=table,
        lam=stiffness(np.arange(extent), extent),
        edges=np.stack([edge, edge * sign]),
        squares=np.stack([edge**2 * (1 + sign), edge**2 * (1 - sign)]),
        dst=dst[:blocks],
        after=dst[1:],
        gaps=np.stack([1 - theta, 1 + theta], axis=1),
    )


def wave_constants(extent, blocks):
    length = extent * blocks
    half = extent // 2
    kind = np.arange(blocks)
    block = np.arange(blocks)
    angle = np.pi * (kind[:, None] * block[None, :] % (2 * blocks)) / blocks
    parity = np.where(block % 2 == 0, 1.0, -1.0)
    mix = np.stack([np.cos(angle), np.where(kind[:, None] > 0, np.sin(angle), parity[None, :])], axis=1)
    first = kind
    second = np.where(kind == 0, blocks, 2 * blocks - kind)
    place = 2 * np.arange(extent) + 1
    phase_one = np.pi * (first[:, None] * place[None, :] % (4 * length)) / (2 * length)
    phase_two = np.pi * (second[:, None] * place[None, :] % (4 * length)) / (2 * length)
    inner = (kind > 0)[:, None] * 1.0
    twiddle = np.stack(
        [
            np.cos(phase_one),
            -inner * np.sin(phase_one),
            -np.sin(phase_one),
            -inner * np.cos(phase_one),
            inner * np.cos(phase_two),
            np.where(kind[:, None] > 0, np.sin(phase_two), np.cos(phase_two)),
            -inner * np.sin(phase_two),
            np.where(kind[:, None] > 0, np.cos(phase_two), -np.sin(phase_two)),
        ],
        axis=1,
    )
    twiddle[0, 2] = 0.0
    steps = np.arange(half)
    fine = np.pi * (steps[None, :] * place[:, None] % (2 * extent)) / extent
    waves = np.stack([first, second], axis=1)[:, :, None] + 2 * blocks * steps[None, None, :]
    energy = np.where(waves == 0, 1.0 / length, 2.0 / length)
    return dict(
        mix=mix,
        twiddle=twiddle,
        fine=np.concatenate([np.cos(fine), np.sin(fine)], axis=0),
        lam=stiffness(waves, length),
        energy=energy,
    )


def f32(table):
    return jnp.asarray(np.asarray(table, np.float32))


def pick(table, index):
    return lax.dynamic_index_in_dim(f32(table), index, 0, keepdims=False)


def gather(payload, axis):
    return lax.all_gather(payload, axis)


def pack(pieces):
    flat = [piece.reshape(-1) for piece in pieces]
    size = sum(piece.shape[0] for piece in flat)
    return jnp.concatenate(flat).reshape(size // LANES, LANES)


def spread(value):
    return jnp.full((LANES,), value)


def body(row_of, col_of, waves_of, field, direction, ground, previous):
    rows, cols = field.shape
    row_count = row_of["dst"].shape[0]
    col_count = col_of["dst"].shape[0]
    half = rows // 2
    me_row = lax.axis_index(ROW)
    me_col = lax.axis_index(COL)
    g = ground[0]

    row_table, col_table = f32(row_of["table"]), f32(col_of["table"])
    top, bottom = f32(row_of["edges"][0])[:, None], f32(row_of["edges"][1])[:, None]
    left, right = f32(col_of["edges"][0])[None, :], f32(col_of["edges"][1])[None, :]

    weight = 1.0 / (f32(row_of["lam"])[:, None] + f32(col_of["lam"])[None, :] + g)
    block = mm(row_table, mm(field, col_table, ((1,), (1,))), ((1,), (0,)))
    solved = weight * block

    sums = mm(f32(row_of["squares"]), weight, ((1,), (0,)))
    gaps = f32(row_of["gaps"])
    row_inverse = 1.0 / (1.0 + gaps[:, :1] * sums[:1] + gaps[:, 1:] * sums[1:])
    lam_here = pick(waves_of["lam"], me_row).reshape(1, rows)
    long_weight = 1.0 / (f32(col_of["lam"])[:, None] + lam_here + g)
    sums = mm(f32(col_of["squares"]), long_weight, ((1,), (0,)))
    gaps = f32(col_of["gaps"])
    col_inverse = pick(waves_of["energy"], me_row).reshape(1, rows) / (
        1.0 + gaps[:, :1] * sums[:1] + gaps[:, 1:] * sums[1:]
    )

    row_edges = mm(f32(row_of["edges"]), solved, ((1,), (0,)))
    col_edges = mm(f32(col_of["edges"]), solved, ((1,), (1,)))
    energy = jnp.sum(solved * block)
    seen = gather(pack([row_edges, col_edges, spread(energy)]), ROW).reshape(row_count, -1)
    tops, bottoms = seen[:, :cols], seen[:, cols : 2 * cols]
    lefts, rights = seen[:, 2 * cols : 2 * cols + rows], seen[:, 2 * cols + rows : 2 * cols + 2 * rows]
    energy = jnp.sum(seen[:, 2 * cols + 2 * rows])

    dst, after = row_of["dst"], row_of["after"]
    jumps = mm(f32(np.concatenate([after.T, -dst.T], axis=1)), jnp.concatenate([bottoms, tops], axis=0), ((1,), (0,)))
    bends = row_inverse * jumps
    energy = energy - jnp.sum(bends * jumps)

    sides = mm(
        jnp.concatenate([bends * left, bends * right], axis=0), weight, ((1,), (1,))
    )
    mix = waves_of["mix"]
    mix_here = pick(np.concatenate([mix, mix @ dst, mix @ after], axis=2), me_row)
    mixed = []
    for which, side in ((0, lefts), (1, rights)):
        part = sides[which * row_count : (which + 1) * row_count]
        mixed.append(
            mm(mix_here[:, :row_count], side, ((1,), (0,)))
            + mm(mix_here[:, row_count : 2 * row_count], part, ((1,), (0,))) * top.T
            - mm(mix_here[:, 2 * row_count :], part, ((1,), (0,))) * bottom.T
        )
    in_place = mm(jnp.concatenate(mixed, axis=0), row_table, ((1,), (0,))).reshape(2, 2, rows)
    real, imag = in_place[:, 0], in_place[:, 1]
    tw = pick(waves_of["twiddle"], me_row)
    fine = f32(waves_of["fine"])
    first = jnp.concatenate([real * tw[0] + imag * tw[1], real * tw[2] + imag * tw[3]], axis=1)
    second = jnp.concatenate([real * tw[4] + imag * tw[5], real * tw[6] + imag * tw[7]], axis=1)
    waves = mm(jnp.concatenate([first, second], axis=0), fine, ((1,), (0,)))
    waves = jnp.concatenate([waves[:2], waves[2:]], axis=1)

    seen = gather(pack([waves, spread(energy)]), COL).reshape(col_count, -1)
    energy = jnp.sum(seen[:, 2 * rows])
    dst_c, after_c = col_of["dst"], col_of["after"]
    leaps = mm(
        f32(np.concatenate([after_c.T, -dst_c.T], axis=1)),
        jnp.concatenate([seen[:, rows : 2 * rows], seen[:, :rows]], axis=0),
        ((1,), (0,)),
    )
    folds = col_inverse * leaps
    fold_energy = jnp.sum(folds * leaps)
    mine = mm(pick(np.stack([dst_c, after_c], axis=1), me_col), folds, ((1,), (0,)))
    back = mm(jnp.concatenate([mine[:, :half], mine[:, half:]], axis=0), fine, ((1,), (1,)))
    c_one, s_one, c_two, s_two = back[:2, :rows], back[:2, rows:], back[2:, :rows], back[2:, rows:]
    real = c_one * tw[0] + s_one * tw[2] + c_two * tw[4] + s_two * tw[6]
    imag = c_one * tw[1] + s_one * tw[3] + c_two * tw[5] + s_two * tw[7]
    hats = mm(jnp.concatenate([real, imag], axis=0), row_table, ((1,), (1,)))

    seen = gather(pack([hats, spread(fold_energy)]), ROW).reshape(row_count, -1)
    energy = energy - jnp.sum(seen[:, 4 * rows])
    parts = seen[:, : 4 * rows].reshape(row_count, 2, 2, rows)
    unmix = np.concatenate([mix[:, 0].T, mix[:, 1].T], axis=1)
    spectra = jnp.concatenate([parts[:, 0], parts[:, 1]], axis=0).reshape(2 * row_count, 2 * rows)
    here = mm(pick(unmix, me_row)[None], spectra, ((1,), (0,)))
    side_left, side_right = here[:, :rows].T, here[:, rows:].T
    pulls = mm(f32(np.concatenate([after.T @ unmix, dst.T @ unmix], axis=0)), spectra, ((1,), (0,)))
    pulls_left = pulls[:row_count, :rows] * bottom.T - pulls[row_count:, :rows] * top.T
    pulls_right = pulls[:row_count, rows:] * bottom.T - pulls[row_count:, rows:] * top.T
    pulled = mm(jnp.concatenate([pulls_left, pulls_right], axis=0), weight, ((1,), (0,)))
    jumps = jumps + left * pulled[:row_count] - right * pulled[row_count:]
    ends = mm(pick(np.stack([dst, after], axis=1), me_row), row_inverse * jumps, ((1,), (0,)))
    spectrum = weight * (
        block + top * ends[:1] - bottom * ends[1:] + side_left * left - side_right * right
    )
    precond = mm(row_table, mm(spectrum, col_table, ((1,), (0,))), ((0,), (0,)))
    ratio = energy / previous[0]
    return precond + ratio * direction, jnp.reshape(ratio, (1,))


def build(row_count, col_count, rows, cols):
    row_of = block_constants(rows, row_count)
    col_of = block_constants(cols, col_count)
    waves_of = wave_constants(rows, row_count)

    def run(field, direction, ground, previous):
        return body(row_of, col_of, waves_of, field, direction, ground, previous)

    return run


def solution(mesh):
    row_count, col_count = mesh.shape[ROW], mesh.shape[COL]

    def step(residual, direction, ground_shift, previous):
        rows, cols = residual.shape[0] // row_count, residual.shape[1] // col_count
        return jax.shard_map(
            build(row_count, col_count, rows, cols),
            mesh=mesh,
            in_specs=(P(ROW, COL), P(ROW, COL), P(), P()),
            out_specs=(P(ROW, COL), P()),
            check_vma=False,
        )(residual, direction, ground_shift, previous)

    return step
```

```python
import numpy as np
import jax
import jax.numpy as jnp
from jax import lax
from jax.sharding import PartitionSpec as P

ROW = "row"
COL = "col"
LANES = 128

HI = lax.Precision.HIGHEST


def mm(a, b, dims):
    return lax.dot_general(a, b, (dims, ((), ())), precision=HI)


def cosines(length):
    wave = np.arange(length)[:, None]
    place = np.arange(length)[None, :]
    angle = np.pi * (wave * (2 * place + 1) % (4 * length)) / (2 * length)
    scale = np.where(wave == 0, np.sqrt(1.0 / length), np.sqrt(2.0 / length))
    return scale * np.cos(angle)


def stiffness(waves, length):
    return 4.0 * np.sin(np.pi * waves / (2 * length)) ** 2


def sines(blocks):
    index = np.arange(blocks + 1)
    table = np.sqrt(2.0 / blocks) * np.sin(np.pi * (index[:, None] * index[None, :] % (2 * blocks)) / blocks)
    table[blocks] = 0.0
    return table[:, :blocks]


def block_constants(extent, blocks):
    table = cosines(extent)
    edge = table[:, 0]
    sign = np.where(np.arange(extent) % 2 == 0, 1.0, -1.0)
    dst = sines(blocks)
    theta = np.cos(np.pi * np.arange(blocks) / blocks)
    return dict(
        table=table,
        lam=stiffness(np.arange(extent), extent),
        edges=np.stack([edge, edge * sign]),
        squares=np.stack([edge**2 * (1 + sign), edge**2 * (1 - sign)]),
        dst=dst[:blocks],
        after=dst[1:],
        gaps=np.stack([1 - theta, 1 + theta], axis=1),
    )


def wave_constants(extent, blocks):
    length = extent * blocks
    half = extent // 2
    kind = np.arange(blocks)
    block = np.arange(blocks)
    angle = np.pi * (kind[:, None] * block[None, :] % (2 * blocks)) / blocks
    parity = np.where(block % 2 == 0, 1.0, -1.0)
    mix = np.stack([np.cos(angle), np.where(kind[:, None] > 0, np.sin(angle), parity[None, :])], axis=1)
    first = kind
    second = np.where(kind == 0, blocks, 2 * blocks - kind)
    place = 2 * np.arange(extent) + 1
    phase_one = np.pi * (first[:, None] * place[None, :] % (4 * length)) / (2 * length)
    phase_two = np.pi * (second[:, None] * place[None, :] % (4 * length)) / (2 * length)
    inner = (kind > 0)[:, None] * 1.0
    twiddle = np.stack(
        [
            np.cos(phase_one),
            -inner * np.sin(phase_one),
            -np.sin(phase_one),
            -inner * np.cos(phase_one),
            inner * np.cos(phase_two),
            np.where(kind[:, None] > 0, np.sin(phase_two), np.cos(phase_two)),
            -inner * np.sin(phase_two),
            np.where(kind[:, None] > 0, np.cos(phase_two), -np.sin(phase_two)),
        ],
        axis=1,
    )
    twiddle[0, 2] = 0.0
    steps = np.arange(half)
    fine = np.pi * (steps[None, :] * place[:, None] % (2 * extent)) / extent
    waves = np.stack([first, second], axis=1)[:, :, None] + 2 * blocks * steps[None, None, :]
    energy = np.where(waves == 0, 1.0 / length, 2.0 / length)
    return dict(
        mix=mix,
        twiddle=twiddle,
        fine=np.concatenate([np.cos(fine), np.sin(fine)], axis=0),
        lam=stiffness(waves, length),
        energy=energy,
    )


def f32(table):
    return jnp.asarray(np.asarray(table, np.float32))


def pick(table, index):
    return lax.dynamic_index_in_dim(f32(table), index, 0, keepdims=False)


def gather(payload, axis):
    copies = jnp.broadcast_to(payload[None], (lax.axis_size(axis),) + payload.shape)
    return lax.all_to_all(copies, axis, 0, 0, tiled=True)


def pack(pieces):
    flat = [piece.reshape(-1) for piece in pieces]
    size = sum(piece.shape[0] for piece in flat)
    full = -(-size // (8 * LANES)) * 8 * LANES
    flat.append(jnp.zeros((full - size,), jnp.float32))
    return jnp.concatenate(flat).reshape(full // LANES, LANES)


def spread(value):
    return jnp.full((LANES,), value)


def body(row_of, col_of, waves_of, field, direction, ground, previous):
    rows, cols = field.shape
    row_count = row_of["dst"].shape[0]
    col_count = col_of["dst"].shape[0]
    half = rows // 2
    me_row = lax.axis_index(ROW)
    me_col = lax.axis_index(COL)
    g = ground[0]

    row_table, col_table = f32(row_of["table"]), f32(col_of["table"])
    top, bottom = f32(row_of["edges"][0])[:, None], f32(row_of["edges"][1])[:, None]
    left, right = f32(col_of["edges"][0])[None, :], f32(col_of["edges"][1])[None, :]

    weight = 1.0 / (f32(row_of["lam"])[:, None] + f32(col_of["lam"])[None, :] + g)
    block = mm(row_table, mm(field, col_table, ((1,), (1,))), ((1,), (0,)))
    solved = weight * block

    sums = mm(f32(row_of["squares"]), weight, ((1,), (0,)))
    gaps = f32(row_of["gaps"])
    row_inverse = 1.0 / (1.0 + gaps[:, :1] * sums[:1] + gaps[:, 1:] * sums[1:])
    lam_here = pick(waves_of["lam"], me_row).reshape(1, rows)
    long_weight = 1.0 / (f32(col_of["lam"])[:, None] + lam_here + g)
    sums = mm(f32(col_of["squares"]), long_weight, ((1,), (0,)))
    gaps = f32(col_of["gaps"])
    col_inverse = pick(waves_of["energy"], me_row).reshape(1, rows) / (
        1.0 + gaps[:, :1] * sums[:1] + gaps[:, 1:] * sums[1:]
    )

    row_edges = mm(f32(row_of["edges"]), solved, ((1,), (0,)))
    col_edges = mm(f32(col_of["edges"]), solved, ((1,), (1,)))
    energy = jnp.sum(solved * block)
    seen = gather(pack([row_edges, col_edges, spread(energy)]), ROW).reshape(row_count, -1)
    tops, bottoms = seen[:, :cols], seen[:, cols : 2 * cols]
    lefts, rights = seen[:, 2 * cols : 2 * cols + rows], seen[:, 2 * cols + rows : 2 * cols + 2 * rows]
    energy = jnp.sum(seen[:, 2 * cols + 2 * rows])

    dst, after = row_of["dst"], row_of["after"]
    jumps = mm(f32(np.concatenate([after.T, -dst.T], axis=1)), jnp.concatenate([bottoms, tops], axis=0), ((1,), (0,)))
    bends = row_inverse * jumps
    energy = energy - jnp.sum(bends * jumps)

    sides = mm(
        jnp.concatenate([bends * left, bends * right], axis=0), weight, ((1,), (1,))
    )
    mix = waves_of["mix"]
    mix_here = pick(np.concatenate([mix, mix @ dst, mix @ after], axis=2), me_row)
    mixed = []
    for which, side in ((0, lefts), (1, rights)):
        part = sides[which * row_count : (which + 1) * row_count]
        mixed.append(
            mm(mix_here[:, :row_count], side, ((1,), (0,)))
            + mm(mix_here[:, row_count : 2 * row_count], part, ((1,), (0,))) * top.T
            - mm(mix_here[:, 2 * row_count :], part, ((1,), (0,))) * bottom.T
        )
    in_place = mm(jnp.concatenate(mixed, axis=0), row_table, ((1,), (0,))).reshape(2, 2, rows)
    real, imag = in_place[:, 0], in_place[:, 1]
    tw = pick(waves_of["twiddle"], me_row)
    fine = f32(waves_of["fine"])
    first = jnp.concatenate([real * tw[0] + imag * tw[1], real * tw[2] + imag * tw[3]], axis=1)
    second = jnp.concatenate([real * tw[4] + imag * tw[5], real * tw[6] + imag * tw[7]], axis=1)
    waves = mm(jnp.concatenate([first, second], axis=0), fine, ((1,), (0,)))
    waves = jnp.concatenate([waves[:2], waves[2:]], axis=1)

    seen = gather(pack([waves, spread(energy)]), COL).reshape(col_count, -1)
    energy = jnp.sum(seen[:, 2 * rows])
    dst_c, after_c = col_of["dst"], col_of["after"]
    leaps = mm(
        f32(np.concatenate([after_c.T, -dst_c.T], axis=1)),
        jnp.concatenate([seen[:, rows : 2 * rows], seen[:, :rows]], axis=0),
        ((1,), (0,)),
    )
    folds = col_inverse * leaps
    fold_energy = jnp.sum(folds * leaps)
    mine = mm(pick(np.stack([dst_c, after_c], axis=1), me_col), folds, ((1,), (0,)))
    back = mm(jnp.concatenate([mine[:, :half], mine[:, half:]], axis=0), fine, ((1,), (1,)))
    c_one, s_one, c_two, s_two = back[:2, :rows], back[:2, rows:], back[2:, :rows], back[2:, rows:]
    real = c_one * tw[0] + s_one * tw[2] + c_two * tw[4] + s_two * tw[6]
    imag = c_one * tw[1] + s_one * tw[3] + c_two * tw[5] + s_two * tw[7]
    hats = mm(jnp.concatenate([real, imag], axis=0), row_table, ((1,), (1,)))

    seen = gather(pack([hats, spread(fold_energy)]), ROW).reshape(row_count, -1)
    energy = energy - jnp.sum(seen[:, 4 * rows])
    parts = seen[:, : 4 * rows].reshape(row_count, 2, 2, rows)
    unmix = np.concatenate([mix[:, 0].T, mix[:, 1].T], axis=1)
    spectra = jnp.concatenate([parts[:, 0], parts[:, 1]], axis=0).reshape(2 * row_count, 2 * rows)
    here = mm(pick(unmix, me_row)[None], spectra, ((1,), (0,)))
    side_left, side_right = here[:, :rows].T, here[:, rows:].T
    pulls = mm(f32(np.concatenate([after.T @ unmix, dst.T @ unmix], axis=0)), spectra, ((1,), (0,)))
    pulls_left = pulls[:row_count, :rows] * bottom.T - pulls[row_count:, :rows] * top.T
    pulls_right = pulls[:row_count, rows:] * bottom.T - pulls[row_count:, rows:] * top.T
    pulled = mm(jnp.concatenate([pulls_left, pulls_right], axis=0), weight, ((1,), (0,)))
    jumps = jumps + left * pulled[:row_count] - right * pulled[row_count:]
    ends = mm(pick(np.stack([dst, after], axis=1), me_row), row_inverse * jumps, ((1,), (0,)))
    spectrum = weight * (
        block + top * ends[:1] - bottom * ends[1:] + side_left * left - side_right * right
    )
    precond = mm(row_table, mm(spectrum, col_table, ((1,), (0,))), ((0,), (0,)))
    ratio = energy / previous[0]
    return precond + ratio * direction, jnp.reshape(ratio, (1,))


def build(row_count, col_count, rows, cols):
    row_of = block_constants(rows, row_count)
    col_of = block_constants(cols, col_count)
    waves_of = wave_constants(rows, row_count)

    def run(field, direction, ground, previous):
        return body(row_of, col_of, waves_of, field, direction, ground, previous)

    return run


def solution(mesh):
    row_count, col_count = mesh.shape[ROW], mesh.shape[COL]

    def step(residual, direction, ground_shift, previous):
        rows, cols = residual.shape[0] // row_count, residual.shape[1] // col_count
        return jax.shard_map(
            build(row_count, col_count, rows, cols),
            mesh=mesh,
            in_specs=(P(ROW, COL), P(ROW, COL), P(), P()),
            out_specs=(P(ROW, COL), P()),
            check_vma=False,
        )(residual, direction, ground_shift, previous)

    return step
```

```python
import numpy as np
import jax
import jax.numpy as jnp
from jax import lax
from jax.experimental import pallas as pl
from jax.experimental.pallas import tpu as pltpu
from jax.sharding import PartitionSpec as P

ROW = "row"
COL = "col"
TILE = 8

HI = lax.Precision.HIGHEST


def cosines(length):
    wave = np.arange(length)[:, None]
    place = np.arange(length)[None, :]
    angle = np.pi * (wave * (2 * place + 1) % (4 * length)) / (2 * length)
    scale = np.where(wave == 0, np.sqrt(1.0 / length), np.sqrt(2.0 / length))
    return scale * np.cos(angle)


def stiffness(waves, length):
    return 4.0 * np.sin(np.pi * waves / (2 * length)) ** 2


def sines(blocks):
    index = np.arange(blocks + 1)
    table = np.sqrt(2.0 / blocks) * np.sin(np.pi * (index[:, None] * index[None, :] % (2 * blocks)) / blocks)
    table[blocks] = 0.0
    return table[:, :blocks]


def block_constants(extent, blocks):
    table = cosines(extent)
    edge = table[:, 0]
    sign = np.where(np.arange(extent) % 2 == 0, 1.0, -1.0)
    dst = sines(blocks)
    theta = np.cos(np.pi * np.arange(blocks) / blocks)
    return dict(
        table=table,
        lam=stiffness(np.arange(extent), extent),
        edges=np.stack([edge, edge * sign]),
        columns=np.stack([edge, edge * sign], axis=1),
        squares=np.stack([edge**2 * (1 + sign), edge**2 * (1 - sign)]),
        dst=dst[:blocks],
        after=dst[1:],
        gaps=np.stack([1 - theta, 1 + theta], axis=1),
    )


def wave_constants(extent, blocks):
    length = extent * blocks
    half = extent // 2
    kind = np.arange(blocks)
    block = np.arange(blocks)
    angle = np.pi * (kind[:, None] * block[None, :] % (2 * blocks)) / blocks
    parity = np.where(block % 2 == 0, 1.0, -1.0)
    mix = np.stack([np.cos(angle), np.where(kind[:, None] > 0, np.sin(angle), parity[None, :])], axis=1)
    first = kind
    second = np.where(kind == 0, blocks, 2 * blocks - kind)
    place = 2 * np.arange(extent) + 1
    phase_one = np.pi * (first[:, None] * place[None, :] % (4 * length)) / (2 * length)
    phase_two = np.pi * (second[:, None] * place[None, :] % (4 * length)) / (2 * length)
    inner = (kind > 0)[:, None] * 1.0
    twiddle = np.stack(
        [
            np.cos(phase_one),
            -inner * np.sin(phase_one),
            -np.sin(phase_one),
            -inner * np.cos(phase_one),
            inner * np.cos(phase_two),
            np.where(kind[:, None] > 0, np.sin(phase_two), np.cos(phase_two)),
            -inner * np.sin(phase_two),
            np.where(kind[:, None] > 0, np.cos(phase_two), -np.sin(phase_two)),
        ],
        axis=1,
    )
    twiddle[0, 2] = 0.0
    steps = np.arange(half)
    fine = np.pi * (steps[None, :] * place[:, None] % (2 * extent)) / extent
    waves = np.stack([first, second], axis=1)[:, :, None] + 2 * blocks * steps[None, None, :]
    energy = np.where(waves == 0, 1.0 / length, 2.0 / length)
    return dict(
        mix=mix,
        twiddle=twiddle,
        fine=np.concatenate([np.cos(fine), np.sin(fine)], axis=0),
        lam=stiffness(waves, length),
        energy=energy,
    )


def rows_of(height, width, placed):
    table = np.zeros((height, width))
    for at, row in placed.items():
        table[at] = row
    return table


def kernel_constants(rows, cols, row_count, col_count):
    row = block_constants(rows, row_count)
    col = block_constants(cols, col_count)
    wave = wave_constants(rows, row_count)
    half = rows // 2
    top, bottom = row["edges"]
    left, right = col["edges"]
    mix, dst, after = wave["mix"], row["dst"], row["after"]
    blank = np.zeros((row_count, row_count))

    send_low = rows_of(TILE, rows, {0: top, 2: bottom})
    send_high = rows_of(TILE, rows, {1: top, 3: bottom})
    send_side = rows_of(TILE, cols, {4: left, 5: right})

    def doubled(per_class):
        none = np.zeros_like(per_class)
        pair = [np.concatenate([per_class, none], 1), np.concatenate([none, per_class], 1)]
        zero = np.zeros((row_count, 2 * row_count))
        return np.stack(pair + pair + [zero] * 4, axis=1)

    classes = np.concatenate(
        [doubled(m) for m in (mix[:, 0], mix[:, 1], mix[:, 0] @ dst, mix[:, 1] @ dst, mix[:, 0] @ after, mix[:, 1] @ after)],
        axis=1,
    )
    dst_c, after_c = col["dst"], col["after"]
    gap = np.zeros((col_count, TILE * col_count))
    leaps_first, leaps_second, sum_energy = gap.copy(), gap.copy(), np.zeros((TILE, TILE * col_count))
    leaps_first[:, 1::TILE], leaps_first[:, 0::TILE] = after_c.T, -dst_c.T
    leaps_second[:, 3::TILE], leaps_second[:, 2::TILE] = after_c.T, -dst_c.T
    sum_energy[:, 4::TILE] = 1.0
    own_c = np.zeros((col_count, 2 * TILE, col_count))
    own_c[:, 0], own_c[:, 1] = dst_c, after_c
    own_c[:, TILE + 2], own_c[:, TILE + 3] = dst_c, after_c

    unmix = np.concatenate([mix[:, 0].T, mix[:, 1].T], axis=1)
    own_r = np.zeros((row_count, 3 * TILE, 2 * row_count))
    own_r[:, 2] = unmix
    own_r[:, TILE + 3] = -unmix
    own_r[:, 2 * TILE, :row_count], own_r[:, 2 * TILE + 1, :row_count] = dst, after
    return dict(
        row_table=row["table"],
        col_table=col["table"],
        row_lam=row["lam"][:, None],
        col_lam=col["lam"][None, :],
        col_lam_down=col["lam"][:, None],
        row_edges=rows_of(TILE, rows, {0: top, 1: bottom}),
        col_edges=rows_of(TILE, cols, {0: left, 1: right}),
        row_squares=rows_of(TILE, rows, {0: row["squares"][0], 1: row["squares"][1]}),
        col_squares=rows_of(TILE, cols, {0: col["squares"][0], 1: col["squares"][1]}),
        row_gaps=row["gaps"],
        col_gaps=col["gaps"],
        send_low=send_low,
        send_high=send_high,
        send_side=send_side,
        jumps=np.concatenate([after.T, -dst.T], axis=1),
        classes=classes,
        twiddle=wave["twiddle"],
        twiddle_all=np.transpose(wave["twiddle"], (1, 0, 2)).reshape(TILE * row_count, rows),
        fine_cos=wave["fine"][:rows],
        fine_sin=wave["fine"][rows:],
        wave_lam=wave["lam"].reshape(row_count, 1, rows),
        wave_energy=wave["energy"].reshape(row_count, 1, rows),
        leaps=np.concatenate([leaps_first, leaps_second, sum_energy], axis=0),
        own_c=own_c,
        pulls=np.concatenate([after.T @ unmix, dst.T @ unmix], axis=0),
        own_r=own_r,
        pair_rows=rows_of(TILE, rows, {0: top, 1: -bottom}),
        pair_cols=rows_of(TILE, cols, {2: left, 3: right}),
    )


def nn(a, b):
    return lax.dot_general(a, b, (((1,), (0,)), ((), ())), precision=HI, preferred_element_type=jnp.float32)


def nt(a, b):
    return lax.dot_general(a, b, (((1,), (1,)), ((), ())), precision=HI, preferred_element_type=jnp.float32)


def tn(a, b):
    return lax.dot_general(a, b, (((0,), (0,)), ((), ())), precision=HI, preferred_element_type=jnp.float32)


def row_number(shape):
    return lax.broadcasted_iota(jnp.int32, shape, 0)


def send_all(out_ref, tile):
    for peer in range(out_ref.shape[0]):
        out_ref[peer] = tile


def edges_kernel(g, field, col_table, row_table, row_lam, col_lam, low, high, side, block_out, weight_out, send_out):
    rows = field.shape[0]
    block = nn(row_table[...], nt(field[...], col_table[...]))
    weight = 1.0 / (row_lam[...] + col_lam[...] + g[0])
    solved = weight * block
    block_out[...] = block
    weight_out[...] = weight
    energy = jnp.sum(solved * block)
    tile = nn(low[...], solved[:, :rows]) + nn(high[...], solved[:, rows:]) + nt(side[...], solved)
    tile = jnp.where(row_number(tile.shape) == 6, energy, tile)
    send_all(send_out, jnp.concatenate([tile[:, : rows // 2], tile[:, rows // 2 :]], axis=0))


def systems_kernel(g, me, weight, row_squares, row_gaps, col_lam, col_squares, col_gaps, wave_lam, wave_energy, row_out, col_out):
    sums = nn(row_squares[...], weight[...])
    row_out[...] = 1.0 / (1.0 + row_gaps[:, 0:1] * sums[0:1] + row_gaps[:, 1:2] * sums[1:2])
    long_weight = 1.0 / (col_lam[...] + wave_lam[me[0]] + g[0])
    sums = nn(col_squares[...], long_weight)
    col_out[...] = wave_energy[me[0]] / (1.0 + col_gaps[:, 0:1] * sums[0:1] + col_gaps[:, 1:2] * sums[1:2])


def classes_kernel(me, seen, weight, row_inverse, jump_table, classes, row_edges, col_edges, row_table, twiddle, fine_cos, fine_sin, jumps_out, send_out):
    count, rows = jump_table.shape[0], weight.shape[0]

    def strided(at):
        parts = [seen[pl.ds(at + side, count, stride=2 * TILE), :] for side in (0, TILE)]
        return jnp.concatenate(parts, axis=1)

    ends_low = jnp.concatenate([strided(2), strided(0)], axis=0)
    ends_high = jnp.concatenate([strided(3), strided(1)], axis=0)
    sides = jnp.concatenate([strided(4), strided(5)], axis=0)
    energy = jnp.sum(strided(6)[:, 0:1])
    jumps = [nn(jump_table[...], ends_low), nn(jump_table[...], ends_high)]
    total = jnp.zeros((), jnp.float32)
    moved = jnp.zeros((2 * count, rows), jnp.float32)
    for half in range(2):
        span = slice(half * rows, (half + 1) * rows)
        jumps_out[:, span] = jumps[half]
        bends = row_inverse[:, span] * jumps[half]
        total = total + jnp.sum(bends * jumps[half])
        both = jnp.concatenate([bends * col_edges[0:1, span], bends * col_edges[1:2, span]], axis=0)
        moved = moved + nt(both, weight[:, span])
    table = classes[me[0]]
    mixed = nn(table[: 2 * TILE], sides)
    bent = nn(table[2 * TILE :], moved)
    mixed = mixed + bent[: 2 * TILE] * row_edges[0:1] - bent[2 * TILE :] * row_edges[1:2]
    placed = nn(mixed, row_table[...])
    real, imag = placed[:TILE], placed[TILE:]
    tw = twiddle[me[0]]
    opening = row_number((TILE, rows)) < 2
    even = real * jnp.where(opening, tw[0:1], tw[4:5]) + imag * jnp.where(opening, tw[1:2], tw[5:6])
    odd = real * jnp.where(opening, tw[2:3], tw[6:7]) + imag * jnp.where(opening, tw[3:4], tw[7:8])
    tile = nn(even, fine_cos[...]) + nn(odd, fine_sin[...])
    send_all(send_out, jnp.where(row_number(tile.shape) == 4, energy - total, tile))


def folds_kernel(me, seen, col_inverse, leaps, own, send_out):
    count, half = col_inverse.shape[0], seen.shape[1]
    out = nn(leaps[...], seen[...])
    first, second = out[:count], out[count : 2 * count]
    fold_first = col_inverse[:, :half] * first
    fold_second = col_inverse[:, half:] * second
    energy = out[2 * count : 2 * count + 1, 0:1] / send_out.shape[0]
    energy = energy - jnp.sum(fold_first * first + fold_second * second)
    table = own[me[0]]
    tile = nn(table[:TILE], fold_first) + nn(table[TILE:], fold_second)
    send_all(send_out, jnp.where(row_number(tile.shape) == 4, energy, tile))


def finish_kernel(previous, me, seen, block, weight, direction, jumps, row_inverse, twiddle, fine_cos, fine_sin, pulls, own, row_edges, col_edges, pair_rows, pair_cols, row_table, col_table, out, ratio_out):
    count = jumps.shape[0]

    def strided(at):
        return seen[pl.ds(at, count, stride=TILE), :]

    waves = jnp.concatenate([strided(0), strided(1), strided(2), strided(3)], axis=0)
    ratio = jnp.sum(strided(4)[:, 0:1]) / previous[0]
    ratio_out[0] = ratio
    even = nt(waves, fine_cos[...])
    odd = nt(waves, fine_sin[...])

    def tw(at):
        return twiddle[at * count : (at + 1) * count]

    spectra = []
    for at in range(2):
        one, two = slice(at * count, (at + 1) * count), slice((at + 2) * count, (at + 3) * count)
        real = even[one] * tw(0) + odd[one] * tw(2) + even[two] * tw(4) + odd[two] * tw(6)
        imag = even[one] * tw(1) + odd[one] * tw(3) + even[two] * tw(5) + odd[two] * tw(7)
        spectra.append(jnp.concatenate([real, imag], axis=0))
    table = own[me[0]]
    mine = nn(table[:TILE], spectra[0]) + nn(table[TILE : 2 * TILE], spectra[1])
    pulled = jnp.concatenate([nn(pulls[...], spectra[0]), nn(pulls[...], spectra[1]), mine], axis=0)
    hats = nt(pulled, row_table[...])
    edge_top, edge_bottom = row_edges[0:1], row_edges[1:2]
    both = jnp.concatenate(
        [
            hats[:count] * edge_bottom - hats[count : 2 * count] * edge_top,
            hats[2 * count : 3 * count] * edge_bottom - hats[3 * count : 4 * count] * edge_top,
        ],
        axis=0,
    )
    mine = hats[4 * count :]
    shifts = nn(both, weight[...])
    jump = jumps[...] + col_edges[0:1] * shifts[:count] - col_edges[1:2] * shifts[count:]
    ends = nn(table[2 * TILE :, :count], row_inverse[...] * jump)
    spectrum = weight[...] * (block[...] + tn(pair_rows[...] + mine, pair_cols[...] + ends))
    out[...] = tn(row_table[...], nn(spectrum, col_table[...])) + ratio * direction[...]


def f32(table):
    return jnp.asarray(np.asarray(table, np.float32))


def call(kernel, name, outs, scalars, arrays, flops, room=16 * 2**20):
    vmem = pl.BlockSpec(memory_space=pltpu.VMEM)
    smem = pl.BlockSpec(memory_space=pltpu.SMEM)
    spaces = [pltpu.SMEM if shape == (1,) else pltpu.VMEM for shape in outs]
    shapes = [space(shape, jnp.float32) for space, shape in zip(spaces, outs)]
    specs = [smem if shape == (1,) else vmem for shape in outs]
    moved = sum(4 * int(np.prod(shape)) for shape in outs) + sum(4 * a.size for a in arrays)
    return pl.pallas_call(
        kernel,
        out_shape=shapes,
        in_specs=[smem] * len(scalars) + [vmem] * len(arrays),
        out_specs=specs,
        name=name,
        compiler_params=pltpu.CompilerParams(vmem_limit_bytes=room),
        cost_estimate=pl.CostEstimate(flops=flops, bytes_accessed=moved, transcendentals=0),
    )(*scalars, *[pltpu.with_memory_space_constraint(a, pltpu.VMEM) for a in arrays])


def exchange(copies, axis):
    seen = lax.all_to_all(copies, axis, 0, 0, tiled=True)
    return seen.reshape(seen.shape[0] * seen.shape[1], seen.shape[2])


def body(of, row_count, col_count, field, direction, ground, previous):
    rows, cols = field.shape
    half = rows // 2
    me_row = lax.axis_index(ROW).reshape(1)
    me_col = lax.axis_index(COL).reshape(1)
    k = {name: f32(table) for name, table in of.items()}

    block, weight, send = call(
        edges_kernel,
        "edges",
        [(rows, cols), (rows, cols), (row_count, 2 * TILE, half)],
        [ground],
        [field, k["col_table"], k["row_table"], k["row_lam"], k["col_lam"], k["send_low"], k["send_high"], k["send_side"]],
        2 * rows * cols * (rows + cols),
    )
    seen = exchange(send, ROW)
    row_inverse, col_inverse = call(
        systems_kernel,
        "systems",
        [(row_count, cols), (col_count, rows)],
        [ground, me_row],
        [weight, k["row_squares"], k["row_gaps"], k["col_lam_down"], k["col_squares"], k["col_gaps"], k["wave_lam"], k["wave_energy"]],
        2 * rows * cols * 32,
    )
    jumps, send = call(
        classes_kernel,
        "classes",
        [(row_count, cols), (col_count, TILE, half)],
        [me_row],
        [seen, weight, row_inverse, k["jumps"], k["classes"], k["row_edges"], k["col_edges"], k["row_table"], k["twiddle"], k["fine_cos"], k["fine_sin"]],
        2 * rows * cols * 128,
    )
    seen = exchange(send, COL)
    (send,) = call(
        folds_kernel,
        "folds",
        [(row_count, TILE, half)],
        [me_col],
        [seen, col_inverse, k["leaps"], k["own_c"]],
        2 * rows * cols * 16,
    )
    seen = exchange(send, ROW)
    out, ratio = call(
        finish_kernel,
        "finish",
        [(rows, cols), (1,)],
        [previous, me_row],
        [seen, block, weight, direction, jumps, row_inverse, k["twiddle_all"], k["fine_cos"], k["fine_sin"], k["pulls"], k["own_r"], k["row_edges"], k["col_edges"], k["pair_rows"], k["pair_cols"], k["row_table"], k["col_table"]],
        2 * rows * cols * (rows + cols + 128),
    )
    return out, ratio


def solution(mesh):
    row_count, col_count = mesh.shape[ROW], mesh.shape[COL]

    def step(residual, direction, ground_shift, previous):
        rows, cols = residual.shape[0] // row_count, residual.shape[1] // col_count
        of = kernel_constants(rows, cols, row_count, col_count)

        def local(field, heading, ground, last):
            return body(of, row_count, col_count, field, heading, ground, last)

        return jax.shard_map(
            local,
            mesh=mesh,
            in_specs=(P(ROW, COL), P(ROW, COL), P(), P()),
            out_specs=(P(ROW, COL), P()),
            check_vma=False,
        )(residual, direction, ground_shift, previous)

    return step
```

```python
import numpy as np
import jax
import jax.numpy as jnp
from jax import lax
from jax.experimental import pallas as pl
from jax.experimental.pallas import tpu as pltpu
from jax.sharding import PartitionSpec as P

ROW = "row"
COL = "col"
TILE = 8
LANES = 128

HI = lax.Precision.HIGHEST


def cosines(length):
    wave = np.arange(length)[:, None]
    place = np.arange(length)[None, :]
    angle = np.pi * (wave * (2 * place + 1) % (4 * length)) / (2 * length)
    scale = np.where(wave == 0, np.sqrt(1.0 / length), np.sqrt(2.0 / length))
    return scale * np.cos(angle)


def stiffness(waves, length):
    return 4.0 * np.sin(np.pi * waves / (2 * length)) ** 2


def sines(blocks):
    index = np.arange(blocks + 1)
    table = np.sqrt(2.0 / blocks) * np.sin(np.pi * (index[:, None] * index[None, :] % (2 * blocks)) / blocks)
    table[blocks] = 0.0
    return table[:, :blocks]


def block_constants(extent, blocks):
    table = cosines(extent)
    edge = table[:, 0]
    sign = np.where(np.arange(extent) % 2 == 0, 1.0, -1.0)
    dst = sines(blocks)
    theta = np.cos(np.pi * np.arange(blocks) / blocks)
    return dict(
        table=table,
        lam=stiffness(np.arange(extent), extent),
        edges=np.stack([edge, edge * sign]),
        columns=np.stack([edge, edge * sign], axis=1),
        squares=np.stack([edge**2 * (1 + sign), edge**2 * (1 - sign)]),
        dst=dst[:blocks],
        after=dst[1:],
        gaps=np.stack([1 - theta, 1 + theta], axis=1),
    )


def wave_constants(extent, blocks):
    length = extent * blocks
    half = extent // 2
    kind = np.arange(blocks)
    block = np.arange(blocks)
    angle = np.pi * (kind[:, None] * block[None, :] % (2 * blocks)) / blocks
    parity = np.where(block % 2 == 0, 1.0, -1.0)
    mix = np.stack([np.cos(angle), np.where(kind[:, None] > 0, np.sin(angle), parity[None, :])], axis=1)
    first = kind
    second = np.where(kind == 0, blocks, 2 * blocks - kind)
    place = 2 * np.arange(extent) + 1
    phase_one = np.pi * (first[:, None] * place[None, :] % (4 * length)) / (2 * length)
    phase_two = np.pi * (second[:, None] * place[None, :] % (4 * length)) / (2 * length)
    inner = (kind > 0)[:, None] * 1.0
    twiddle = np.stack(
        [
            np.cos(phase_one),
            -inner * np.sin(phase_one),
            -np.sin(phase_one),
            -inner * np.cos(phase_one),
            inner * np.cos(phase_two),
            np.where(kind[:, None] > 0, np.sin(phase_two), np.cos(phase_two)),
            -inner * np.sin(phase_two),
            np.where(kind[:, None] > 0, np.cos(phase_two), -np.sin(phase_two)),
        ],
        axis=1,
    )
    twiddle[0, 2] = 0.0
    steps = np.arange(half)
    fine = np.pi * (steps[None, :] * place[:, None] % (2 * extent)) / extent
    waves = np.stack([first, second], axis=1)[:, :, None] + 2 * blocks * steps[None, None, :]
    energy = np.where(waves == 0, 1.0 / length, 2.0 / length)
    return dict(
        mix=mix,
        twiddle=twiddle,
        fine=np.concatenate([np.cos(fine), np.sin(fine)], axis=0),
        lam=stiffness(waves, length),
        energy=energy,
    )


def kernel_constants(rows, cols, row_count, col_count):
    row = block_constants(rows, row_count)
    col = block_constants(cols, col_count)
    wave = wave_constants(rows, row_count)
    half = rows // 2
    top, bottom = row["edges"]
    left, right = col["edges"]
    mix, dst, after = wave["mix"], row["dst"], row["after"]
    dst_c, after_c = col["dst"], col["after"]
    unmix = np.concatenate([mix[:, 0].T, mix[:, 1].T], axis=1)

    columns = np.zeros((rows, LANES))
    columns[:, 0] = row["lam"]
    for piece in range(cols // rows):
        columns[:, 8 + piece] = col["lam"][piece * rows : (piece + 1) * rows]
    columns[:row_count, 1:3] = row["gaps"]
    columns[:col_count, 3:5] = col["gaps"]

    sends = np.zeros((3 * TILE, cols))
    sends[0, :rows] = sends[1, rows : 2 * rows] = top
    sends[2, :rows] = sends[3, rows : 2 * rows] = bottom
    sends[TILE + 4], sends[TILE + 5] = left, right
    sends[2 * TILE] = col["lam"]

    small = np.zeros((2 * row_count + 5 * TILE, max(3 * LANES, 2 * rows, cols)))
    small[: 2 * row_count, : 2 * row_count] = np.concatenate([after.T @ unmix, dst.T @ unmix], axis=0)
    small[:row_count, LANES : LANES + 2 * row_count] = np.concatenate([after.T, -dst.T], axis=1)
    small[:row_count, 2 * LANES : 2 * LANES + row_count] = dst
    small[row_count : 2 * row_count, 2 * LANES : 2 * LANES + row_count] = after
    base = 2 * row_count
    small[base, :rows], small[base + 1, :rows] = top, bottom
    small[base, rows : 2 * rows], small[base + 1, rows : 2 * rows] = top, -bottom
    small[base + TILE, :cols], small[base + TILE + 1, :cols] = left, right
    small[base + 2 * TILE : base + 2 * TILE + 2, :rows] = row["squares"]
    small[base + 3 * TILE : base + 3 * TILE + 2, :cols] = col["squares"]
    small[base + 4 * TILE + 2, :cols], small[base + 4 * TILE + 3, :cols] = left, right

    leaps = np.zeros((2 * col_count + TILE, TILE * col_count))
    reach = max(LANES, TILE * col_count)
    leaps[:col_count, 1::TILE], leaps[:col_count, 0::TILE] = after_c.T, -dst_c.T
    leaps[col_count : 2 * col_count, 3::TILE], leaps[col_count : 2 * col_count, 2::TILE] = after_c.T, -dst_c.T
    leaps[2 * col_count, 4::TILE] = 1.0
    own_c = np.zeros((TILE * col_count, col_count))
    for at in (0, 2):
        own_c[at::TILE], own_c[at + 1 :: TILE] = dst_c, after_c

    classes = np.zeros((row_count, 2 * TILE, max(rows, 2 * row_count)))
    classes[:, :TILE, :rows] = wave["twiddle"]
    classes[:, 8, :rows] = wave["lam"].reshape(row_count, rows)
    classes[:, 9, :rows] = wave["energy"].reshape(row_count, rows)
    classes[:, 10, :row_count], classes[:, 11, :row_count] = mix[:, 0], mix[:, 1]
    classes[:, 12, : 2 * row_count] = unmix
    classes[:, 13, :row_count], classes[:, 14, :row_count] = dst, after
    slabs = [classes[:, :, :half], classes[:, :, half:rows]]
    return dict(
        row_table=row["table"],
        col_table=col["table"],
        columns=columns,
        sends=sends,
        small=small,
        leaps=np.concatenate(
            [np.pad(table, ((0, 0), (0, reach - table.shape[1]))) for table in (own_c, leaps)], axis=0
        ),
        classes=np.concatenate([slab.reshape(2 * TILE * row_count, half) for slab in slabs], axis=0),
        fine=np.concatenate([wave["fine"][:rows], wave["fine"][rows:]], axis=1),
    )


def nn(a, b):
    return lax.dot_general(a, b, (((1,), (0,)), ((), ())), precision=HI, preferred_element_type=jnp.float32)


def nt(a, b):
    return lax.dot_general(a, b, (((1,), (1,)), ((), ())), precision=HI, preferred_element_type=jnp.float32)


def tn(a, b):
    return lax.dot_general(a, b, (((0,), (0,)), ((), ())), precision=HI, preferred_element_type=jnp.float32)


def row_number(shape):
    return lax.broadcasted_iota(jnp.int32, shape, 0)


def send_all(out_ref, copies_ref, sent, tile):
    for peer in range(out_ref.shape[0]):
        copies_ref[peer] = tile
    copy = pltpu.make_async_copy(copies_ref, out_ref, sent)
    copy.start()
    copy.wait()


def aligned(index, size):
    return pl.ds(pl.multiple_of(index * size, size), size)


def class_rows(classes, me, first):
    start = pl.multiple_of(me * 2 * TILE, TILE) + first
    slab = classes.shape[0] // 2
    return jnp.concatenate([classes[pl.ds(start, TILE), :], classes[pl.ds(slab + start, TILE), :]], axis=1)


def edges_kernel(g, field, col_table, row_table, columns, sends, block_out, weight_out, send_out, field_in, col_in, row_in, columns_in, sends_in, arrived, block_here, copies_here, left_core):
    rows = field.shape[0]
    pairs = [(row_table, row_in), (field, field_in), (columns, columns_in), (sends, sends_in), (col_table, col_in)]
    copies = [pltpu.make_async_copy(src, dst, arrived.at[at]) for at, (src, dst) in enumerate(pairs)]
    for copy in copies:
        copy.start()
    copies[0].wait()
    copies[1].wait()
    halfway = nn(row_in[...], field_in[...])
    copies[2].wait()
    copies[3].wait()
    weight = 1.0 / (columns_in[:, 0:1] + sends_in[2 * TILE : 2 * TILE + 1] + g[0])
    weight_out[...] = weight
    copies[4].wait()
    block = nt(halfway, col_in[...])
    solved = weight * block
    block_here[...] = block
    keep = pltpu.make_async_copy(block_here, block_out, left_core.at[0])
    keep.start()
    energy = jnp.sum(solved * block)
    low, side = sends_in[:TILE], sends_in[TILE : 2 * TILE]
    tile = nn(low[:, :rows], solved[:, :rows]) + nn(low[:, rows:], solved[:, rows:]) + nt(side, solved)
    tile = jnp.where(row_number(tile.shape) == 6, energy, tile)
    tile = jnp.concatenate([tile[:, : rows // 2], tile[:, rows // 2 :]], axis=0)
    send_all(send_out, copies_here, left_core.at[1], tile)
    keep.wait()


def make_kernels(row_count, col_count, rows, cols):
    base = 2 * row_count
    half = rows // 2

    def systems_kernel(g, me, weight, columns, small, classes, out):
        sums = nn(small[base + 2 * TILE : base + 3 * TILE, :rows], weight[...])
        gaps = columns[:row_count, 1:3]
        out[:row_count] = 1.0 / (1.0 + gaps[:, 0:1] * sums[0:1] + gaps[:, 1:2] * sums[1:2])
        mine = class_rows(classes, me[0], TILE)
        down = jnp.concatenate([columns[:, 8 + piece : 9 + piece] for piece in range(cols // rows)], axis=0)
        long_weight = 1.0 / (down + mine[0:1] + g[0])
        sums = nn(small[base + 3 * TILE : base + 4 * TILE, :cols], long_weight)
        gaps = columns[:col_count, 3:5]
        out[row_count : row_count + col_count, :rows] = mine[1:2] / (1.0 + gaps[:, 0:1] * sums[0:1] + gaps[:, 1:2] * sums[1:2])
        sines_here = small[:base, 2 * LANES : 2 * LANES + row_count]
        out[row_count : row_count + TILE, rows : rows + row_count] = nn(mine[:, :row_count], sines_here[:row_count])
        out[row_count + TILE : row_count + 2 * TILE, rows : rows + row_count] = nn(mine[:, :row_count], sines_here[row_count:])

    def classes_kernel(me, seen, weight, systems, row_table, fine, small, classes, jumps_out, send_out, jumps_here, copies_here, left_core):
        def strided(at):
            parts = [seen[pl.ds(at + side, row_count, stride=2 * TILE), :] for side in (0, TILE)]
            return jnp.concatenate(parts, axis=1)

        lows = jnp.concatenate([strided(2), strided(0)], axis=0)
        highs = jnp.concatenate([strided(3), strided(1)], axis=0)
        jump_table = small[:row_count, LANES : LANES + 2 * row_count]
        jumps = nn(jump_table, jnp.concatenate([lows, highs], axis=1))
        jumps_here[...] = jumps
        keep = pltpu.make_async_copy(jumps_here, jumps_out, left_core.at[0])
        keep.start()
        bends = systems[:row_count] * jumps
        energy = jnp.sum(strided(6)[:, 0:1]) - jnp.sum(bends * jumps)
        lefts, rights = small[base + TILE : base + TILE + 1, :cols], small[base + TILE + 1 : base + TILE + 2, :cols]
        moved = nt(jnp.concatenate([bends * lefts, bends * rights], axis=0), weight[...])
        moved = jnp.concatenate([moved[:row_count], moved[row_count:]], axis=1)
        mine = class_rows(classes, me[0], TILE)[:, :row_count]
        mixed = nn(mine, jnp.concatenate([strided(4), strided(5)], axis=1))
        top, bottom = small[base : base + 1, :rows], small[base + 1 : base + 2, :rows]
        bent = nn(systems[row_count : row_count + 2 * TILE, rows : rows + row_count], moved)
        mixed = (
            mixed
            + bent[:TILE] * jnp.concatenate([top, top], axis=1)
            - bent[TILE : 2 * TILE] * jnp.concatenate([bottom, bottom], axis=1)
        )
        placed = nn(jnp.concatenate([mixed[:, :rows], mixed[:, rows:]], axis=0), row_table[...])
        number = row_number((TILE, rows))
        lefty = lax.rem(number, 2) == 0
        real = jnp.where(lefty, placed[2:3], placed[TILE + 2 : TILE + 3])
        imag = jnp.where(lefty, placed[3:4], placed[TILE + 3 : TILE + 4])
        tw = class_rows(classes, me[0], 0)
        opening = number < 2
        even = real * jnp.where(opening, tw[0:1], tw[4:5]) + imag * jnp.where(opening, tw[1:2], tw[5:6])
        odd = real * jnp.where(opening, tw[2:3], tw[6:7]) + imag * jnp.where(opening, tw[3:4], tw[7:8])
        tile = nn(even, fine[:, :half]) + nn(odd, fine[:, half:])
        send_all(send_out, copies_here, left_core.at[1], jnp.where(row_number(tile.shape) == 4, energy, tile))
        keep.wait()

    def folds_kernel(me, seen, systems, leaps, send_out, copies_here, left_core):
        skip = TILE * col_count
        out = nn(leaps[skip:, :skip], seen[...])
        first, second = out[:col_count], out[col_count : 2 * col_count]
        fold_first = systems[row_count : row_count + col_count, :half] * first
        fold_second = systems[row_count : row_count + col_count, half:rows] * second
        energy = out[2 * col_count : 2 * col_count + 1, 0:1] / row_count
        energy = energy - jnp.sum(fold_first * first + fold_second * second)
        table = leaps[aligned(me[0], TILE), :col_count]
        tile = jnp.where(row_number((TILE, half)) < 2, nn(table, fold_first), nn(table, fold_second))
        send_all(send_out, copies_here, left_core.at[0], jnp.where(row_number(tile.shape) == 4, energy, tile))

    def finish_kernel(previous, me, seen, weight, systems, fine, small, classes, row_table, jumps, block, col_table, direction, out, ratio_out, jumps_in, block_in, col_in, direction_in, arrived, ready, left_core):
        pairs = [(jumps, jumps_in), (block, block_in), (col_table, col_in), (direction, direction_in)]
        loads = [pltpu.make_async_copy(src, dst, arrived.at[at]) for at, (src, dst) in enumerate(pairs)]
        for load in loads:
            load.start()

        def strided(at):
            return seen[pl.ds(at, row_count, stride=TILE), :]

        def tw(at):
            slab = classes.shape[0] // 2
            parts = [classes[pl.ds(at + side, row_count, stride=2 * TILE), :] for side in (0, slab)]
            return jnp.concatenate(parts, axis=1)

        waves = jnp.concatenate([strided(0), strided(1), strided(2), strided(3)], axis=0)
        ratio = jnp.sum(strided(4)[:, 0:1]) / previous[0]
        ratio_out[0] = ratio
        even = nt(waves, fine[:, :half])
        odd = nt(waves, fine[:, half:])
        spectra = []
        for at in range(2):
            one, two = slice(at * row_count, (at + 1) * row_count), slice((at + 2) * row_count, (at + 3) * row_count)
            real = even[one] * tw(0) + odd[one] * tw(2) + even[two] * tw(4) + odd[two] * tw(6)
            imag = even[one] * tw(1) + odd[one] * tw(3) + even[two] * tw(5) + odd[two] * tw(7)
            spectra.append(jnp.concatenate([real, imag], axis=0))
        mine = class_rows(classes, me[0], TILE)
        table = jnp.concatenate([small[:base, :base], mine[:, :base]], axis=0)
        pulled = nn(table, jnp.concatenate(spectra, axis=1))
        hats = nt(jnp.concatenate([pulled[:, :rows], pulled[:, rows:]], axis=0), row_table[...])
        top, bottom = small[base : base + 1, :rows], small[base + 1 : base + 2, :rows]
        skip = base + TILE
        both = jnp.concatenate(
            [
                hats[:row_count] * bottom - hats[row_count:base] * top,
                hats[skip : skip + row_count] * bottom - hats[skip + row_count : skip + base] * top,
            ],
            axis=0,
        )
        own_left, own_right = hats[base + 4 : base + 5], hats[skip + base + 4 : skip + base + 5]
        shifts = nn(both, weight[...])
        lefts, rights = small[base + TILE : base + TILE + 1, :cols], small[base + TILE + 1 : base + TILE + 2, :cols]
        loads[0].wait()
        jump = jumps_in[...] + lefts * shifts[:row_count] - rights * shifts[row_count:]
        ends = nn(mine[:, :row_count], systems[:row_count] * jump)
        number = row_number((TILE, rows))
        down = jnp.where(number == 2, own_left, jnp.where(number == 3, -own_right, small[base : base + TILE, rows : 2 * rows]))
        number = row_number((TILE, cols))
        along = jnp.where(number == 0, ends[5:6], jnp.where(number == 1, ends[6:7], small[base + 4 * TILE : base + 5 * TILE, :cols]))
        down = jnp.where(row_number(down.shape) < 4, down, 0.0)
        loads[1].wait()
        spectrum = weight[...] * (block_in[...] + tn(down, along))
        loads[2].wait()
        halfway = nn(spectrum, col_in[...])
        loads[3].wait()
        step = max(cols // 4, half)
        copies = []
        for at in range(cols // step):
            span = slice(at * step, (at + 1) * step)
            ready[:, span] = tn(row_table[...], halfway[:, span]) + ratio * direction_in[:, span]
            copy = pltpu.make_async_copy(ready.at[:, span], out.at[:, span], left_core.at[at])
            copy.start()
            copies.append(copy)
        for copy in copies:
            copy.wait()

    return systems_kernel, classes_kernel, folds_kernel, finish_kernel


def f32(table):
    return jnp.asarray(np.asarray(table, np.float32))


def call(kernel, name, outs, scalars, arrays, flops, scratch=(), room=16 * 2**20):
    spaces = dict(vmem=pltpu.VMEM, hbm=pltpu.HBM, window=pltpu.VMEM, smem=pltpu.SMEM)

    def shape_of(shape, kind):
        made = dict(vmem=pltpu.VMEM, hbm=pltpu.HBM).get(kind, jax.ShapeDtypeStruct)
        return made(shape, jnp.float32)

    def placed(array, kind):
        return array if kind == "window" else pltpu.with_memory_space_constraint(array, spaces[kind])

    moved = sum(4 * int(np.prod(shape)) for shape, _ in outs) + sum(4 * a.size for a, _ in arrays)
    return pl.pallas_call(
        kernel,
        out_shape=[shape_of(*entry) for entry in outs],
        in_specs=[pl.BlockSpec(memory_space=pltpu.SMEM)] * len(scalars)
        + [pl.BlockSpec(memory_space=spaces[kind]) for _, kind in arrays],
        out_specs=[pl.BlockSpec(memory_space=spaces[kind]) for _, kind in outs],
        scratch_shapes=list(scratch),
        name=name,
        compiler_params=pltpu.CompilerParams(vmem_limit_bytes=room),
        cost_estimate=pl.CostEstimate(flops=flops, bytes_accessed=moved, transcendentals=0),
    )(*scalars, *[placed(*entry) for entry in arrays])


def exchange(copies, axis):
    seen = lax.all_to_all(copies, axis, 0, 0, tiled=True)
    return seen.reshape(seen.shape[0] * seen.shape[1], seen.shape[2])


def body(of, row_count, col_count, field, direction, ground, previous):
    rows, cols = field.shape
    half = rows // 2
    me_row = lax.axis_index(ROW).reshape(1)
    me_col = lax.axis_index(COL).reshape(1)
    k = {name: f32(table) for name, table in of.items()}
    systems_kernel, classes_kernel, folds_kernel, finish_kernel = make_kernels(row_count, col_count, rows, cols)

    def space(shape):
        return pltpu.VMEM(shape, jnp.float32)

    two = pltpu.SemaphoreType.DMA((2,))

    def hold(*arrays):
        return [(array, "vmem") for array in arrays]

    loads = (field, k["col_table"], k["row_table"], k["columns"], k["sends"])
    block, weight, send = call(
        edges_kernel,
        "edges",
        [((rows, cols), "hbm"), ((rows, cols), "vmem"), ((row_count, 2 * TILE, half), "hbm")],
        [ground],
        [(array, "hbm") for array in loads],
        2 * rows * cols * (rows + cols),
        [space(array.shape) for array in loads]
        + [pltpu.SemaphoreType.DMA((len(loads),)), space((rows, cols)), space((row_count, 2 * TILE, half)), two],
    )
    seen = exchange(send, ROW)
    (systems,) = call(
        systems_kernel,
        "systems",
        [((row_count + max(col_count, 2 * TILE), cols), "window")],
        [ground, me_row],
        hold(weight, k["columns"], k["small"], k["classes"]),
        2 * rows * cols * 32,
    )
    jumps, send = call(
        classes_kernel,
        "classes",
        [((row_count, cols), "hbm"), ((col_count, TILE, half), "hbm")],
        [me_row],
        hold(seen, weight, systems, k["row_table"], k["fine"], k["small"], k["classes"]),
        2 * rows * cols * 128,
        [space((row_count, cols)), space((col_count, TILE, half)), two],
    )
    seen = exchange(send, COL)
    (send,) = call(
        folds_kernel,
        "folds",
        [((row_count, TILE, half), "hbm")],
        [me_col],
        hold(seen, systems, k["leaps"]),
        2 * rows * cols * 16,
        [space((row_count, TILE, half)), two],
    )
    seen = exchange(send, ROW)
    late = (jumps, block, k["col_table"], direction)
    out, ratio = call(
        finish_kernel,
        "finish",
        [((rows, cols), "hbm"), ((1,), "smem")],
        [previous, me_row],
        hold(seen, weight, systems, k["fine"], k["small"], k["classes"], k["row_table"])
        + [(array, "hbm") for array in late],
        2 * rows * cols * (rows + cols + 128),
        [space(array.shape) for array in late]
        + [pltpu.SemaphoreType.DMA((len(late),)), space((rows, cols)), pltpu.SemaphoreType.DMA((4,))],
    )
    return out, ratio


def solution(mesh):
    row_count, col_count = mesh.shape[ROW], mesh.shape[COL]

    def step(residual, direction, ground_shift, previous):
        rows, cols = residual.shape[0] // row_count, residual.shape[1] // col_count
        of = kernel_constants(rows, cols, row_count, col_count)

        def local(field, heading, ground, last):
            return body(of, row_count, col_count, field, heading, ground, last)

        return jax.shard_map(
            local,
            mesh=mesh,
            in_specs=(P(ROW, COL), P(ROW, COL), P(), P()),
            out_specs=(P(ROW, COL), P()),
            check_vma=False,
        )(residual, direction, ground_shift, previous)

    return step
```

```python
import numpy as np
import jax
import jax.numpy as jnp
from jax import lax
from jax.experimental import pallas as pl
from jax.experimental.pallas import tpu as pltpu
from jax.sharding import PartitionSpec as P

ROW = "row"
COL = "col"
TILE = 8
LANES = 128

HI = lax.Precision.HIGHEST


def cosines(length):
    wave = np.arange(length)[:, None]
    place = np.arange(length)[None, :]
    angle = np.pi * (wave * (2 * place + 1) % (4 * length)) / (2 * length)
    scale = np.where(wave == 0, np.sqrt(1.0 / length), np.sqrt(2.0 / length))
    return scale * np.cos(angle)


def stiffness(waves, length):
    return 4.0 * np.sin(np.pi * waves / (2 * length)) ** 2


def sines(blocks):
    index = np.arange(blocks + 1)
    table = np.sqrt(2.0 / blocks) * np.sin(np.pi * (index[:, None] * index[None, :] % (2 * blocks)) / blocks)
    table[blocks] = 0.0
    return table[:, :blocks]


def block_constants(extent, blocks):
    table = cosines(extent)
    edge = table[:, 0]
    sign = np.where(np.arange(extent) % 2 == 0, 1.0, -1.0)
    dst = sines(blocks)
    theta = np.cos(np.pi * np.arange(blocks) / blocks)
    return dict(
        table=table,
        lam=stiffness(np.arange(extent), extent),
        edges=np.stack([edge, edge * sign]),
        columns=np.stack([edge, edge * sign], axis=1),
        squares=np.stack([edge**2 * (1 + sign), edge**2 * (1 - sign)]),
        dst=dst[:blocks],
        after=dst[1:],
        gaps=np.stack([1 - theta, 1 + theta], axis=1),
    )


def wave_constants(extent, blocks):
    length = extent * blocks
    half = extent // 2
    kind = np.arange(blocks)
    block = np.arange(blocks)
    angle = np.pi * (kind[:, None] * block[None, :] % (2 * blocks)) / blocks
    parity = np.where(block % 2 == 0, 1.0, -1.0)
    mix = np.stack([np.cos(angle), np.where(kind[:, None] > 0, np.sin(angle), parity[None, :])], axis=1)
    first = kind
    second = np.where(kind == 0, blocks, 2 * blocks - kind)
    place = 2 * np.arange(extent) + 1
    phase_one = np.pi * (first[:, None] * place[None, :] % (4 * length)) / (2 * length)
    phase_two = np.pi * (second[:, None] * place[None, :] % (4 * length)) / (2 * length)
    inner = (kind > 0)[:, None] * 1.0
    twiddle = np.stack(
        [
            np.cos(phase_one),
            -inner * np.sin(phase_one),
            -np.sin(phase_one),
            -inner * np.cos(phase_one),
            inner * np.cos(phase_two),
            np.where(kind[:, None] > 0, np.sin(phase_two), np.cos(phase_two)),
            -inner * np.sin(phase_two),
            np.where(kind[:, None] > 0, np.cos(phase_two), -np.sin(phase_two)),
        ],
        axis=1,
    )
    twiddle[0, 2] = 0.0
    steps = np.arange(half)
    fine = np.pi * (steps[None, :] * place[:, None] % (2 * extent)) / extent
    waves = np.stack([first, second], axis=1)[:, :, None] + 2 * blocks * steps[None, None, :]
    energy = np.where(waves == 0, 1.0 / length, 2.0 / length)
    return dict(
        mix=mix,
        twiddle=twiddle,
        fine=np.concatenate([np.cos(fine), np.sin(fine)], axis=0),
        lam=stiffness(waves, length),
        energy=energy,
    )


def kernel_constants(rows, cols, row_count, col_count):
    row = block_constants(rows, row_count)
    col = block_constants(cols, col_count)
    wave = wave_constants(rows, row_count)
    half = rows // 2
    top, bottom = row["edges"]
    left, right = col["edges"]
    mix, dst, after = wave["mix"], row["dst"], row["after"]
    dst_c, after_c = col["dst"], col["after"]
    unmix = np.concatenate([mix[:, 0].T, mix[:, 1].T], axis=1)

    columns = np.zeros((rows, LANES))
    columns[:, 0] = row["lam"]
    columns[:, 5] = top
    for piece in range(cols // rows):
        columns[:, 8 + piece] = col["lam"][piece * rows : (piece + 1) * rows]
    columns[:row_count, 1:3] = row["gaps"]
    columns[:col_count, 3:5] = col["gaps"]

    sends = np.zeros((3 * TILE, cols))
    group = min(LANES, cols)
    sends[4, :group] = 1.0
    sends[5, :group] = np.where(np.arange(group) % 2 == 0, 1.0, -1.0)
    sends[2 * TILE + 1] = left
    sends[2 * TILE] = col["lam"]

    small = np.zeros((2 * row_count + 5 * TILE, max(3 * LANES, 2 * rows, cols)))
    small[: 2 * row_count, : 2 * row_count] = np.concatenate([after.T @ unmix, dst.T @ unmix], axis=0)
    small[:row_count, LANES : LANES + 2 * row_count] = np.concatenate([after.T, -dst.T], axis=1)
    small[:row_count, 2 * LANES : 2 * LANES + row_count] = dst
    small[row_count : 2 * row_count, 2 * LANES : 2 * LANES + row_count] = after
    base = 2 * row_count
    small[base, :rows], small[base + 1, :rows] = top, bottom
    small[base, rows : 2 * rows], small[base + 1, rows : 2 * rows] = top, -bottom
    small[base + TILE, :cols], small[base + TILE + 1, :cols] = left, right
    small[base + 2 * TILE : base + 2 * TILE + 2, :rows] = row["squares"]
    small[base + 3 * TILE : base + 3 * TILE + 2, :cols] = col["squares"]
    small[base + 4 * TILE + 2, :cols], small[base + 4 * TILE + 3, :cols] = left, right

    leaps = np.zeros((2 * col_count + TILE, TILE * col_count))
    reach = max(LANES, TILE * col_count)
    leaps[:col_count, 1::TILE], leaps[:col_count, 0::TILE] = after_c.T, -dst_c.T
    leaps[col_count : 2 * col_count, 3::TILE], leaps[col_count : 2 * col_count, 2::TILE] = after_c.T, -dst_c.T
    leaps[2 * col_count, 4::TILE] = 1.0
    own_c = np.zeros((TILE * col_count, col_count))
    for at in (0, 2):
        own_c[at::TILE], own_c[at + 1 :: TILE] = dst_c, after_c

    classes = np.zeros((row_count, 2 * TILE, max(rows, 2 * row_count)))
    classes[:, :TILE, :rows] = wave["twiddle"]
    classes[:, 8, :rows] = wave["lam"].reshape(row_count, rows)
    classes[:, 9, :rows] = wave["energy"].reshape(row_count, rows)
    classes[:, 10, :row_count], classes[:, 11, :row_count] = mix[:, 0], mix[:, 1]
    classes[:, 12, : 2 * row_count] = unmix
    classes[:, 13, :row_count], classes[:, 14, :row_count] = dst, after
    slabs = [classes[:, :, :half], classes[:, :, half:rows]]
    return dict(
        row_table=row["table"],
        col_table=col["table"],
        columns=columns,
        sends=sends,
        small=small,
        leaps=np.concatenate(
            [np.pad(table, ((0, 0), (0, reach - table.shape[1]))) for table in (own_c, leaps)], axis=0
        ),
        classes=np.concatenate([slab.reshape(2 * TILE * row_count, half) for slab in slabs], axis=0),
        fine=wave["fine"],
    )


def nn(a, b):
    return lax.dot_general(a, b, (((1,), (0,)), ((), ())), precision=HI, preferred_element_type=jnp.float32)


def nt(a, b):
    return lax.dot_general(a, b, (((1,), (1,)), ((), ())), precision=HI, preferred_element_type=jnp.float32)


def halves(a):
    high = a.astype(jnp.bfloat16)
    return high, (a - high.astype(jnp.float32)).astype(jnp.bfloat16)


def three(a, b, dims):
    def dot(x, y):
        return lax.dot_general(x, y, (dims, ((), ())), preferred_element_type=jnp.float32)

    (a_high, a_low), (b_high, b_low) = halves(a), halves(b)
    return dot(a_high, b_high) + (dot(a_high, b_low) + dot(a_low, b_high))


def tn(a, b):
    return lax.dot_general(a, b, (((0,), (0,)), ((), ())), precision=HI, preferred_element_type=jnp.float32)


def row_number(shape):
    return lax.broadcasted_iota(jnp.int32, shape, 0)


def send_all(out_ref, copies_ref, sent, tile):
    for peer in range(out_ref.shape[0]):
        copies_ref[peer] = tile
    copy = pltpu.make_async_copy(copies_ref, out_ref, sent)
    copy.start()
    copy.wait()


def aligned(index, size):
    return pl.ds(pl.multiple_of(index * size, size), size)


def class_rows(classes, me, first):
    start = pl.multiple_of(me * 2 * TILE, TILE) + first
    slab = classes.shape[0] // 2
    return jnp.concatenate([classes[pl.ds(start, TILE), :], classes[pl.ds(slab + start, TILE), :]], axis=1)


def edges_kernel(g, field, col_table, row_table, columns, sends, block_out, weight_out, send_out, field_in, col_in, row_in, columns_in, sends_in, arrived, block_here, copies_here, left_core):
    rows, cols = field.shape
    pairs = [(row_table, row_in), (field, field_in), (columns, columns_in), (sends, sends_in), (col_table, col_in)]
    copies = [pltpu.make_async_copy(src, dst, arrived.at[at]) for at, (src, dst) in enumerate(pairs)]
    for copy in copies:
        copy.start()
    copies[0].wait()
    copies[1].wait()
    halfway = three(row_in[...], field_in[...], ((1,), (0,)))
    copies[2].wait()
    copies[3].wait()
    weight = 1.0 / (columns_in[:, 0:1] + sends_in[2 * TILE : 2 * TILE + 1] + g[0])
    weight_out[...] = weight
    copies[4].wait()
    block = three(halfway, col_in[...], ((1,), (1,)))
    solved = weight * block
    block_here[...] = block
    keep = pltpu.make_async_copy(block_here, block_out, left_core.at[0])
    keep.start()
    energy = jnp.sum(solved * block)
    number = row_number((TILE, rows))
    folded = jnp.sum((solved * columns_in[:, 5:6]).reshape(rows // TILE, TILE, cols), axis=0)
    tops = jnp.sum(folded, axis=0, keepdims=True)
    bottoms = jnp.sum(jnp.where(row_number(folded.shape) % 2 == 0, folded, -folded), axis=0, keepdims=True)
    sided = solved * sends_in[2 * TILE + 1 : 2 * TILE + 2]
    group = min(LANES, cols)
    sided = sum(sided[:, at : at + group] for at in range(0, cols, group))
    tile = nt(sends_in[:TILE, :group], sided)
    tile = jnp.where(number == 0, tops[:, :rows], jnp.where(number == 1, tops[:, rows:], tile))
    tile = jnp.where(number == 2, bottoms[:, :rows], jnp.where(number == 3, bottoms[:, rows:], tile))
    tile = jnp.where(row_number(tile.shape) == 6, energy, tile)
    tile = jnp.concatenate([tile[:, : rows // 2], tile[:, rows // 2 :]], axis=0)
    send_all(send_out, copies_here, left_core.at[1], tile)
    keep.wait()


def make_kernels(row_count, col_count, rows, cols):
    base = 2 * row_count
    half = rows // 2

    def systems_kernel(g, me, weight, columns, small, classes, out):
        sums = nn(small[base + 2 * TILE : base + 3 * TILE, :rows], weight[...])
        gaps = columns[:row_count, 1:3]
        out[:row_count] = 1.0 / (1.0 + gaps[:, 0:1] * sums[0:1] + gaps[:, 1:2] * sums[1:2])
        mine = class_rows(classes, me[0], TILE)
        down = jnp.concatenate([columns[:, 8 + piece : 9 + piece] for piece in range(cols // rows)], axis=0)
        long_weight = 1.0 / (down + mine[0:1] + g[0])
        sums = nn(small[base + 3 * TILE : base + 4 * TILE, :cols], long_weight)
        gaps = columns[:col_count, 3:5]
        out[row_count : row_count + col_count, :rows] = mine[1:2] / (1.0 + gaps[:, 0:1] * sums[0:1] + gaps[:, 1:2] * sums[1:2])
        sines_here = small[:base, 2 * LANES : 2 * LANES + row_count]
        out[row_count : row_count + TILE, rows : rows + row_count] = nn(mine[:, :row_count], sines_here[:row_count])
        out[row_count + TILE : row_count + 2 * TILE, rows : rows + row_count] = nn(mine[:, :row_count], sines_here[row_count:])

    def classes_kernel(me, seen, weight, systems, row_table, fine, small, classes, jumps_out, send_out, jumps_here, copies_here, left_core):
        def strided(at):
            parts = [seen[pl.ds(at + side, row_count, stride=2 * TILE), :] for side in (0, TILE)]
            return jnp.concatenate(parts, axis=1)

        lows = jnp.concatenate([strided(2), strided(0)], axis=0)
        highs = jnp.concatenate([strided(3), strided(1)], axis=0)
        jump_table = small[:row_count, LANES : LANES + 2 * row_count]
        jumps = nn(jump_table, jnp.concatenate([lows, highs], axis=1))
        jumps_here[...] = jumps
        keep = pltpu.make_async_copy(jumps_here, jumps_out, left_core.at[0])
        keep.start()
        bends = systems[:row_count] * jumps
        energy = jnp.sum(strided(6)[:, 0:1]) - jnp.sum(bends * jumps)
        lefts, rights = small[base + TILE : base + TILE + 1, :cols], small[base + TILE + 1 : base + TILE + 2, :cols]
        moved = nt(jnp.concatenate([bends * lefts, bends * rights], axis=0), weight[...])
        moved = jnp.concatenate([moved[:row_count], moved[row_count:]], axis=1)
        mine = class_rows(classes, me[0], TILE)[:, :row_count]
        mixed = nn(mine, jnp.concatenate([strided(4), strided(5)], axis=1))
        top, bottom = small[base : base + 1, :rows], small[base + 1 : base + 2, :rows]
        bent = nn(systems[row_count : row_count + 2 * TILE, rows : rows + row_count], moved)
        mixed = (
            mixed
            + bent[:TILE] * jnp.concatenate([top, top], axis=1)
            - bent[TILE : 2 * TILE] * jnp.concatenate([bottom, bottom], axis=1)
        )
        placed = nn(jnp.concatenate([mixed[:, :rows], mixed[:, rows:]], axis=0), row_table[...])
        number = row_number((TILE, rows))
        lefty = lax.rem(number, 2) == 0
        real = jnp.where(lefty, placed[2:3], placed[TILE + 2 : TILE + 3])
        imag = jnp.where(lefty, placed[3:4], placed[TILE + 3 : TILE + 4])
        tw = class_rows(classes, me[0], 0)
        opening = number < 2
        even = real * jnp.where(opening, tw[0:1], tw[4:5]) + imag * jnp.where(opening, tw[1:2], tw[5:6])
        odd = real * jnp.where(opening, tw[2:3], tw[6:7]) + imag * jnp.where(opening, tw[3:4], tw[7:8])
        tile = nn(jnp.concatenate([even, odd], axis=1), fine[...])
        send_all(send_out, copies_here, left_core.at[1], jnp.where(row_number(tile.shape) == 4, energy, tile))
        keep.wait()

    def folds_kernel(me, seen, systems, leaps, send_out, copies_here, left_core):
        skip = TILE * col_count
        out = nn(leaps[skip:, :skip], seen[...])
        first, second = out[:col_count], out[col_count : 2 * col_count]
        fold_first = systems[row_count : row_count + col_count, :half] * first
        fold_second = systems[row_count : row_count + col_count, half:rows] * second
        energy = out[2 * col_count : 2 * col_count + 1, 0:1] / row_count
        energy = energy - jnp.sum(fold_first * first + fold_second * second)
        table = leaps[aligned(me[0], TILE), :col_count]
        tile = jnp.where(row_number((TILE, half)) < 2, nn(table, fold_first), nn(table, fold_second))
        send_all(send_out, copies_here, left_core.at[0], jnp.where(row_number(tile.shape) == 4, energy, tile))

    def finish_kernel(previous, me, seen, weight, systems, fine, small, classes, row_table, jumps, block, col_table, direction, out, ratio_out, jumps_in, block_in, col_in, direction_in, arrived, ready, left_core):
        pairs = [(jumps, jumps_in), (block, block_in), (col_table, col_in), (direction, direction_in)]
        loads = [pltpu.make_async_copy(src, dst, arrived.at[at]) for at, (src, dst) in enumerate(pairs)]
        for load in loads:
            load.start()

        def strided(at):
            return seen[pl.ds(at, row_count, stride=TILE), :]

        def tw(at):
            slab = classes.shape[0] // 2
            parts = [classes[pl.ds(at + side, row_count, stride=2 * TILE), :] for side in (0, slab)]
            return jnp.concatenate(parts, axis=1)

        waves = jnp.concatenate([strided(0), strided(1), strided(2), strided(3)], axis=0)
        ratio = jnp.sum(strided(4)[:, 0:1]) / previous[0]
        ratio_out[0] = ratio
        both = nt(waves, fine[...])
        even, odd = both[:, :rows], both[:, rows:]
        spectra = []
        for at in range(2):
            one, two = slice(at * row_count, (at + 1) * row_count), slice((at + 2) * row_count, (at + 3) * row_count)
            real = even[one] * tw(0) + odd[one] * tw(2) + even[two] * tw(4) + odd[two] * tw(6)
            imag = even[one] * tw(1) + odd[one] * tw(3) + even[two] * tw(5) + odd[two] * tw(7)
            spectra.append(jnp.concatenate([real, imag], axis=0))
        mine = class_rows(classes, me[0], TILE)
        table = jnp.concatenate([small[:base, :base], mine[:, :base]], axis=0)
        pulled = nn(table, jnp.concatenate(spectra, axis=1))
        hats = nt(jnp.concatenate([pulled[:, :rows], pulled[:, rows:]], axis=0), row_table[...])
        top, bottom = small[base : base + 1, :rows], small[base + 1 : base + 2, :rows]
        skip = base + TILE
        both = jnp.concatenate(
            [
                hats[:row_count] * bottom - hats[row_count:base] * top,
                hats[skip : skip + row_count] * bottom - hats[skip + row_count : skip + base] * top,
            ],
            axis=0,
        )
        own_left, own_right = hats[base + 4 : base + 5], hats[skip + base + 4 : skip + base + 5]
        shifts = nn(both, weight[...])
        lefts, rights = small[base + TILE : base + TILE + 1, :cols], small[base + TILE + 1 : base + TILE + 2, :cols]
        loads[0].wait()
        jump = jumps_in[...] + lefts * shifts[:row_count] - rights * shifts[row_count:]
        ends = nn(mine[:, :row_count], systems[:row_count] * jump)
        number = row_number((TILE, rows))
        down = jnp.where(number == 2, own_left, jnp.where(number == 3, -own_right, small[base : base + TILE, rows : 2 * rows]))
        number = row_number((TILE, cols))
        along = jnp.where(number == 0, ends[5:6], jnp.where(number == 1, ends[6:7], small[base + 4 * TILE : base + 5 * TILE, :cols]))
        down = jnp.where(row_number(down.shape) < 4, down, 0.0)
        loads[1].wait()
        spectrum = weight[...] * (block_in[...] + tn(down, along))
        loads[2].wait()
        halfway = three(spectrum, col_in[...], ((1,), (0,)))
        loads[3].wait()
        copies = []
        for at in range(2):
            span = slice(at * rows // 2, (at + 1) * rows // 2)
            ready[span] = three(row_table[:, span], halfway, ((0,), (0,))) + ratio * direction_in[span]
            copy = pltpu.make_async_copy(ready.at[span], out.at[span], left_core.at[at])
            copy.start()
            copies.append(copy)
        for copy in copies:
            copy.wait()

    return systems_kernel, classes_kernel, folds_kernel, finish_kernel


def f32(table):
    return jnp.asarray(np.asarray(table, np.float32))


def call(kernel, name, outs, scalars, arrays, flops, scratch=(), room=16 * 2**20):
    spaces = dict(vmem=pltpu.VMEM, hbm=pltpu.HBM, window=pltpu.VMEM, smem=pltpu.SMEM)

    def shape_of(shape, kind):
        made = dict(vmem=pltpu.VMEM, hbm=pltpu.HBM).get(kind, jax.ShapeDtypeStruct)
        return made(shape, jnp.float32)

    def placed(array, kind):
        return array if kind == "window" else pltpu.with_memory_space_constraint(array, spaces[kind])

    moved = sum(4 * int(np.prod(shape)) for shape, _ in outs) + sum(4 * a.size for a, _ in arrays)
    return pl.pallas_call(
        kernel,
        out_shape=[shape_of(*entry) for entry in outs],
        in_specs=[pl.BlockSpec(memory_space=pltpu.SMEM)] * len(scalars)
        + [pl.BlockSpec(memory_space=spaces[kind]) for _, kind in arrays],
        out_specs=[pl.BlockSpec(memory_space=spaces[kind]) for _, kind in outs],
        scratch_shapes=list(scratch),
        name=name,
        compiler_params=pltpu.CompilerParams(vmem_limit_bytes=room),
        cost_estimate=pl.CostEstimate(flops=flops, bytes_accessed=moved, transcendentals=0),
    )(*scalars, *[placed(*entry) for entry in arrays])


def exchange(copies, axis):
    seen = lax.all_to_all(copies, axis, 0, 0, tiled=True)
    return seen.reshape(seen.shape[0] * seen.shape[1], seen.shape[2])


def body(of, row_count, col_count, field, direction, ground, previous):
    rows, cols = field.shape
    half = rows // 2
    me_row = lax.axis_index(ROW).reshape(1)
    me_col = lax.axis_index(COL).reshape(1)
    k = {name: f32(table) for name, table in of.items()}
    systems_kernel, classes_kernel, folds_kernel, finish_kernel = make_kernels(row_count, col_count, rows, cols)

    def space(shape):
        return pltpu.VMEM(shape, jnp.float32)

    two = pltpu.SemaphoreType.DMA((2,))

    def hold(*arrays):
        return [(array, "vmem") for array in arrays]

    loads = (field, k["col_table"], k["row_table"], k["columns"], k["sends"])
    block, weight, send = call(
        edges_kernel,
        "edges",
        [((rows, cols), "hbm"), ((rows, cols), "vmem"), ((row_count, 2 * TILE, half), "hbm")],
        [ground],
        [(array, "hbm") for array in loads],
        2 * rows * cols * (rows + cols),
        [space(array.shape) for array in loads]
        + [pltpu.SemaphoreType.DMA((len(loads),)), space((rows, cols)), space((row_count, 2 * TILE, half)), two],
    )
    seen = exchange(send, ROW)
    (systems,) = call(
        systems_kernel,
        "systems",
        [((row_count + max(col_count, 2 * TILE), cols), "window")],
        [ground, me_row],
        hold(weight, k["columns"], k["small"], k["classes"]),
        2 * rows * cols * 32,
    )
    jumps, send = call(
        classes_kernel,
        "classes",
        [((row_count, cols), "hbm"), ((col_count, TILE, half), "hbm")],
        [me_row],
        hold(seen, weight, systems, k["row_table"], k["fine"], k["small"], k["classes"]),
        2 * rows * cols * 128,
        [space((row_count, cols)), space((col_count, TILE, half)), two],
    )
    seen = exchange(send, COL)
    (send,) = call(
        folds_kernel,
        "folds",
        [((row_count, TILE, half), "hbm")],
        [me_col],
        hold(seen, systems, k["leaps"]),
        2 * rows * cols * 16,
        [space((row_count, TILE, half)), two],
    )
    seen = exchange(send, ROW)
    late = (jumps, block, k["col_table"], direction)
    out, ratio = call(
        finish_kernel,
        "finish",
        [((rows, cols), "hbm"), ((1,), "smem")],
        [previous, me_row],
        hold(seen, weight, systems, k["fine"], k["small"], k["classes"], k["row_table"])
        + [(array, "hbm") for array in late],
        2 * rows * cols * (rows + cols + 128),
        [space(array.shape) for array in late]
        + [pltpu.SemaphoreType.DMA((len(late),)), space((rows, cols)), pltpu.SemaphoreType.DMA((4,))],
    )
    return out, ratio


def solution(mesh):
    row_count, col_count = mesh.shape[ROW], mesh.shape[COL]

    def step(residual, direction, ground_shift, previous):
        rows, cols = residual.shape[0] // row_count, residual.shape[1] // col_count
        of = kernel_constants(rows, cols, row_count, col_count)

        def local(field, heading, ground, last):
            return body(of, row_count, col_count, field, heading, ground, last)

        return jax.shard_map(
            local,
            mesh=mesh,
            in_specs=(P(ROW, COL), P(ROW, COL), P(), P()),
            out_specs=(P(ROW, COL), P()),
            check_vma=False,
        )(residual, direction, ground_shift, previous)

    return step
```

```python
import numpy as np
import jax
import jax.numpy as jnp
from jax import lax
from jax.experimental import pallas as pl
from jax.experimental.pallas import tpu as pltpu
from jax.sharding import Mesh
from jax.sharding import PartitionSpec as P

ROW = ("pair", "core")
PAIR, CORE, COL = "pair", "core", "col"
TILE = 8
WAVES = 5
LANES = 128

HI = lax.Precision.HIGHEST


def cosines(length):
    wave = np.arange(length)[:, None]
    place = np.arange(length)[None, :]
    angle = np.pi * (wave * (2 * place + 1) % (4 * length)) / (2 * length)
    scale = np.where(wave == 0, np.sqrt(1.0 / length), np.sqrt(2.0 / length))
    return scale * np.cos(angle)


def stiffness(waves, length):
    return 4.0 * np.sin(np.pi * waves / (2 * length)) ** 2


def sines(blocks):
    index = np.arange(blocks + 1)
    table = np.sqrt(2.0 / blocks) * np.sin(np.pi * (index[:, None] * index[None, :] % (2 * blocks)) / blocks)
    table[blocks] = 0.0
    return table[:, :blocks]


def block_constants(extent, blocks):
    table = cosines(extent)
    edge = table[:, 0]
    sign = np.where(np.arange(extent) % 2 == 0, 1.0, -1.0)
    dst = sines(blocks)
    theta = np.cos(np.pi * np.arange(blocks) / blocks)
    return dict(
        table=table,
        lam=stiffness(np.arange(extent), extent),
        edges=np.stack([edge, edge * sign]),
        columns=np.stack([edge, edge * sign], axis=1),
        squares=np.stack([edge**2 * (1 + sign), edge**2 * (1 - sign)]),
        dst=dst[:blocks],
        after=dst[1:],
        gaps=np.stack([1 - theta, 1 + theta], axis=1),
    )


def wave_constants(extent, blocks):
    length = extent * blocks
    half = extent // 2
    kind = np.arange(blocks)
    block = np.arange(blocks)
    angle = np.pi * (kind[:, None] * block[None, :] % (2 * blocks)) / blocks
    parity = np.where(block % 2 == 0, 1.0, -1.0)
    mix = np.stack([np.cos(angle), np.where(kind[:, None] > 0, np.sin(angle), parity[None, :])], axis=1)
    first = kind
    second = np.where(kind == 0, blocks, 2 * blocks - kind)
    place = 2 * np.arange(extent) + 1
    phase_one = np.pi * (first[:, None] * place[None, :] % (4 * length)) / (2 * length)
    phase_two = np.pi * (second[:, None] * place[None, :] % (4 * length)) / (2 * length)
    inner = (kind > 0)[:, None] * 1.0
    twiddle = np.stack(
        [
            np.cos(phase_one),
            -inner * np.sin(phase_one),
            -np.sin(phase_one),
            -inner * np.cos(phase_one),
            inner * np.cos(phase_two),
            np.where(kind[:, None] > 0, np.sin(phase_two), np.cos(phase_two)),
            -inner * np.sin(phase_two),
            np.where(kind[:, None] > 0, np.cos(phase_two), -np.sin(phase_two)),
        ],
        axis=1,
    )
    twiddle[0, 2] = 0.0
    steps = np.arange(half)
    fine = np.pi * (steps[None, :] * place[:, None] % (2 * extent)) / extent
    waves = np.stack([first, second], axis=1)[:, :, None] + 2 * blocks * steps[None, None, :]
    energy = np.where(waves == 0, 1.0 / length, 2.0 / length)
    return dict(
        mix=mix,
        twiddle=twiddle,
        fine=np.concatenate([np.cos(fine), np.sin(fine)], axis=0),
        lam=stiffness(waves, length),
        energy=energy,
    )


def kernel_constants(rows, cols, row_count, col_count):
    row = block_constants(rows, row_count)
    col = block_constants(cols, col_count)
    wave = wave_constants(rows, row_count)
    half = rows // 2
    top, bottom = row["edges"]
    left, right = col["edges"]
    mix, dst, after = wave["mix"], row["dst"], row["after"]
    dst_c, after_c = col["dst"], col["after"]
    unmix = np.concatenate([mix[:, 0].T, mix[:, 1].T], axis=1)

    order = np.concatenate([np.arange(0, row_count, 2), np.arange(1, row_count, 2)])
    columns = np.zeros((rows, LANES))
    columns[:, 0] = row["lam"]
    columns[:, 5] = top
    for piece in range(cols // rows):
        columns[:, 8 + piece] = col["lam"][piece * rows : (piece + 1) * rows]
    columns[:row_count, 1:3] = row["gaps"]
    columns[:col_count, 3:5] = col["gaps"]

    sends = np.zeros((3 * TILE, cols))
    group = min(LANES, cols)
    sends[4, :group] = 1.0
    sends[5, :group] = np.where(np.arange(group) % 2 == 0, 1.0, -1.0)
    sends[2 * TILE + 1] = left
    sends[2 * TILE] = col["lam"]

    small = np.zeros((2 * row_count + 5 * TILE, max(3 * LANES, 2 * rows, cols)))
    small[: 2 * row_count, : 2 * row_count] = np.concatenate([after.T @ unmix, dst.T @ unmix], axis=0)
    small[:row_count, LANES : LANES + 2 * row_count] = np.concatenate([after.T[:, order], -dst.T[:, order]], axis=1)
    small[:row_count, 2 * LANES : 2 * LANES + row_count] = dst
    small[row_count : 2 * row_count, 2 * LANES : 2 * LANES + row_count] = after
    base = 2 * row_count
    small[base, :rows], small[base + 1, :rows] = top, bottom
    small[base, rows : 2 * rows], small[base + 1, rows : 2 * rows] = top, -bottom
    small[base + TILE, :cols], small[base + TILE + 1, :cols] = left, right
    small[base + 2 * TILE : base + 2 * TILE + 2, :rows] = row["squares"]
    small[base + 3 * TILE : base + 3 * TILE + 2, :cols] = col["squares"]
    small[base + 4 * TILE + 2, :cols], small[base + 4 * TILE + 3, :cols] = left, right

    leaps = np.zeros((2 * col_count + TILE, TILE * col_count))
    reach = max(LANES, TILE * col_count)
    leaps[:col_count, 1::TILE], leaps[:col_count, 0::TILE] = after_c.T, -dst_c.T
    leaps[col_count : 2 * col_count, 3::TILE], leaps[col_count : 2 * col_count, 2::TILE] = after_c.T, -dst_c.T
    leaps[2 * col_count, 4::TILE] = 1.0
    own_c = np.zeros((TILE * col_count, col_count))
    for at in (0, 2):
        own_c[at::TILE], own_c[at + 1 :: TILE] = dst_c, after_c

    classes = np.zeros((row_count, 2 * TILE, max(rows, 2 * row_count)))
    classes[:, :TILE, :rows] = wave["twiddle"]
    classes[:, 8, :rows] = wave["lam"].reshape(row_count, rows)
    classes[:, 9, :rows] = wave["energy"].reshape(row_count, rows)
    classes[:, 10, :row_count], classes[:, 11, :row_count] = mix[:, 0], mix[:, 1]
    classes[:, 10, half : half + row_count], classes[:, 11, half : half + row_count] = mix[:, 0][:, order], mix[:, 1][:, order]
    classes[:, 12, : 2 * row_count] = unmix
    classes[:, 13, :row_count], classes[:, 14, :row_count] = dst, after
    slabs = [classes[:, :, :half], classes[:, :, half:rows]]
    return dict(
        row_table=row["table"],
        col_table=col["table"],
        columns=columns,
        sends=sends,
        small=small,
        leaps=np.concatenate(
            [np.pad(table, ((0, 0), (0, reach - table.shape[1]))) for table in (own_c, leaps)], axis=0
        ),
        classes=np.concatenate([slab.reshape(2 * TILE * row_count, half) for slab in slabs], axis=0),
        fine=wave["fine"],
    )


def nn(a, b):
    return lax.dot_general(a, b, (((1,), (0,)), ((), ())), precision=HI, preferred_element_type=jnp.float32)


def nt(a, b):
    return lax.dot_general(a, b, (((1,), (1,)), ((), ())), precision=HI, preferred_element_type=jnp.float32)


def halves(a):
    high = a.astype(jnp.bfloat16)
    return high, (a - high.astype(jnp.float32)).astype(jnp.bfloat16)


def three(a, b, dims):
    def dot(x, y):
        return lax.dot_general(x, y, (dims, ((), ())), preferred_element_type=jnp.float32)

    (a_high, a_low), (b_high, b_low) = halves(a), halves(b)
    return dot(a_high, b_high) + (dot(a_high, b_low) + dot(a_low, b_high))


def thirds(a):
    high = a.astype(jnp.bfloat16).astype(jnp.float32)
    rest = a - high
    middle = rest.astype(jnp.bfloat16).astype(jnp.float32)
    return high, middle, rest - middle


def outer(a, b):
    (a_one, a_two, a_three), (b_one, b_two, b_three) = thirds(a), thirds(b)
    left = jnp.concatenate([a_one, a_one, a_two, a_one, a_two, a_three], axis=0).astype(jnp.bfloat16)
    right = jnp.concatenate([b_one, b_two, b_one, b_three, b_two, b_one], axis=0).astype(jnp.bfloat16)
    return lax.dot_general(left, right, (((0,), (0,)), ((), ())), preferred_element_type=jnp.float32)


def row_number(shape):
    return lax.broadcasted_iota(jnp.int32, shape, 0)


def send_all(out_ref, copies_ref, sent, tile):
    for peer in range(out_ref.shape[0]):
        copies_ref[peer] = tile
    copy = pltpu.make_async_copy(copies_ref, out_ref, sent)
    copy.start()
    copy.wait()


def aligned(index, size):
    return pl.ds(pl.multiple_of(index * size, size), size)


def class_rows(classes, me, first):
    start = pl.multiple_of(me * 2 * TILE, TILE) + first
    slab = classes.shape[0] // 2
    return jnp.concatenate([classes[pl.ds(start, TILE), :], classes[pl.ds(slab + start, TILE), :]], axis=1)


def edges_kernel(g, field, col_table, row_table, columns, sends, block_out, weight_out, send_out, field_in, col_in, row_in, columns_in, sends_in, arrived, block_here, copies_here, left_core):
    rows, cols = field.shape
    pairs = [(row_table, row_in), (field, field_in), (columns, columns_in), (sends, sends_in), (col_table, col_in)]
    copies = [pltpu.make_async_copy(src, dst, arrived.at[at]) for at, (src, dst) in enumerate(pairs)]
    for copy in copies:
        copy.start()
    copies[0].wait()
    copies[1].wait()
    halfway = three(row_in[...], field_in[...], ((1,), (0,)))
    copies[2].wait()
    copies[3].wait()
    weight = 1.0 / (columns_in[:, 0:1] + sends_in[2 * TILE : 2 * TILE + 1] + g[0])
    weight_out[...] = weight
    copies[4].wait()
    block = three(halfway, col_in[...], ((1,), (1,)))
    solved = weight * block
    block_here[...] = block
    keep = pltpu.make_async_copy(block_here, block_out, left_core.at[0])
    keep.start()
    energy = jnp.sum(solved * block)
    number = row_number((TILE, rows))
    folded = jnp.sum((solved * columns_in[:, 5:6]).reshape(rows // TILE, TILE, cols), axis=0)
    tops = jnp.sum(folded, axis=0, keepdims=True)
    bottoms = jnp.sum(jnp.where(row_number(folded.shape) % 2 == 0, folded, -folded), axis=0, keepdims=True)
    sided = solved * sends_in[2 * TILE + 1 : 2 * TILE + 2]
    group = min(LANES, cols)
    sided = sum(sided[:, at : at + group] for at in range(0, cols, group))
    tile = nt(sends_in[:TILE, :group], sided)
    tile = jnp.where(number == 0, tops[:, :rows], jnp.where(number == 1, tops[:, rows:], tile))
    tile = jnp.where(number == 2, bottoms[:, :rows], jnp.where(number == 3, bottoms[:, rows:], tile))
    tile = jnp.where(row_number(tile.shape) == 6, energy, tile)
    tile = jnp.concatenate([tile[:, : rows // 2], tile[:, rows // 2 :]], axis=0)
    send_all(send_out, copies_here, left_core.at[1], tile)
    keep.wait()


def make_kernels(row_count, col_count, rows, cols):
    base = 2 * row_count
    half = rows // 2

    def systems_kernel(g, me, weight, columns, small, classes, out):
        sums = nn(small[base + 2 * TILE : base + 3 * TILE, :rows], weight[...])
        gaps = columns[:row_count, 1:3]
        out[:row_count] = 1.0 / (1.0 + gaps[:, 0:1] * sums[0:1] + gaps[:, 1:2] * sums[1:2])
        mine = class_rows(classes, me[0], TILE)
        down = jnp.concatenate([columns[:, 8 + piece : 9 + piece] for piece in range(cols // rows)], axis=0)
        long_weight = 1.0 / (down + mine[0:1] + g[0])
        sums = nn(small[base + 3 * TILE : base + 4 * TILE, :cols], long_weight)
        gaps = columns[:col_count, 3:5]
        out[row_count : row_count + col_count, :rows] = mine[1:2] / (1.0 + gaps[:, 0:1] * sums[0:1] + gaps[:, 1:2] * sums[1:2])
        sines_here = small[:base, 2 * LANES : 2 * LANES + row_count]
        out[row_count : row_count + TILE, rows : rows + row_count] = nn(mine[:, :row_count], sines_here[:row_count])
        out[row_count + TILE : row_count + 2 * TILE, rows : rows + row_count] = nn(mine[:, :row_count], sines_here[row_count:])

    def classes_kernel(me, seen, weight, systems, row_table, fine, small, classes, jumps_out, send_out, jumps_here, copies_here, left_core):
        def strided(at):
            parts = [seen[pl.ds(at + side, row_count, stride=2 * TILE), :] for side in (0, TILE)]
            return jnp.concatenate(parts, axis=1)

        lows = jnp.concatenate([strided(2), strided(0)], axis=0)
        highs = jnp.concatenate([strided(3), strided(1)], axis=0)
        jump_table = small[:row_count, LANES : LANES + 2 * row_count]
        jumps = nn(jump_table, jnp.concatenate([lows, highs], axis=1))
        jumps_here[...] = jumps
        keep = pltpu.make_async_copy(jumps_here, jumps_out, left_core.at[0])
        keep.start()
        bends = systems[:row_count] * jumps
        energy = jnp.sum(strided(6)[:, 0:1]) - jnp.sum(bends * jumps)
        lefts, rights = small[base + TILE : base + TILE + 1, :cols], small[base + TILE + 1 : base + TILE + 2, :cols]
        moved = nt(jnp.concatenate([bends * lefts, bends * rights], axis=0), weight[...])
        moved = jnp.concatenate([moved[:row_count], moved[row_count:]], axis=1)
        mine = class_rows(classes, me[0], TILE)[:, half : half + row_count]
        mixed = nn(mine, jnp.concatenate([strided(4), strided(5)], axis=1))
        top, bottom = small[base : base + 1, :rows], small[base + 1 : base + 2, :rows]
        bent = nn(systems[row_count : row_count + 2 * TILE, rows : rows + row_count], moved)
        mixed = (
            mixed
            + bent[:TILE] * jnp.concatenate([top, top], axis=1)
            - bent[TILE : 2 * TILE] * jnp.concatenate([bottom, bottom], axis=1)
        )
        placed = nn(jnp.concatenate([mixed[:, :rows], mixed[:, rows:]], axis=0), row_table[...])
        number = row_number((TILE, rows))
        lefty = lax.rem(number, 2) == 0
        real = jnp.where(lefty, placed[2:3], placed[TILE + 2 : TILE + 3])
        imag = jnp.where(lefty, placed[3:4], placed[TILE + 3 : TILE + 4])
        tw = class_rows(classes, me[0], 0)
        opening = number < 2
        even = real * jnp.where(opening, tw[0:1], tw[4:5]) + imag * jnp.where(opening, tw[1:2], tw[5:6])
        odd = real * jnp.where(opening, tw[2:3], tw[6:7]) + imag * jnp.where(opening, tw[3:4], tw[7:8])
        tile = nn(jnp.concatenate([even, odd], axis=1), fine[...])
        send_all(send_out, copies_here, left_core.at[1], jnp.where(row_number(tile.shape) == 4, energy, tile))
        keep.wait()

    def folds_kernel(me, seen, systems, leaps, send_out, copies_here, left_core):
        skip = TILE * col_count
        out = nn(leaps[skip:, :skip], seen[...])
        first, second = out[:col_count], out[col_count : 2 * col_count]
        fold_first = systems[row_count : row_count + col_count, :half] * first
        fold_second = systems[row_count : row_count + col_count, half:rows] * second
        energy = out[2 * col_count : 2 * col_count + 1, 0:1] / row_count
        energy = energy - jnp.sum(fold_first * first + fold_second * second)
        table = leaps[aligned(me[0], TILE), :col_count]
        tile = jnp.where(row_number((TILE, half)) < 2, nn(table, fold_first), nn(table, fold_second))
        tile = jnp.where(row_number(tile.shape) == 4, energy, tile)
        for peer in range(row_count):
            copies_here[pl.ds(peer * WAVES, WAVES), :] = tile[:WAVES]
        copy = pltpu.make_async_copy(copies_here, send_out, left_core.at[0])
        copy.start()
        copy.wait()

    def finish_kernel(previous, me, seen, weight, systems, fine, small, classes, row_table, jumps, block, col_table, direction, out, ratio_out, jumps_in, block_in, col_in, direction_in, arrived, ready, left_core):
        pairs = [(jumps, jumps_in), (block, block_in), (col_table, col_in), (direction, direction_in)]
        loads = [pltpu.make_async_copy(src, dst, arrived.at[at]) for at, (src, dst) in enumerate(pairs)]
        for load in loads:
            load.start()

        def strided(at):
            return seen[pl.ds(at, row_count, stride=WAVES), :]

        def tw(at):
            slab = classes.shape[0] // 2
            parts = [classes[pl.ds(at + side, row_count, stride=2 * TILE), :] for side in (0, slab)]
            return jnp.concatenate(parts, axis=1)

        waves = jnp.concatenate([strided(0), strided(1), strided(2), strided(3)], axis=0)
        ratio = jnp.sum(strided(4)[:, 0:1]) / previous[0]
        ratio_out[0] = ratio
        both = nt(waves, fine[...])
        even, odd = both[:, :rows], both[:, rows:]
        spectra = []
        for at in range(2):
            one, two = slice(at * row_count, (at + 1) * row_count), slice((at + 2) * row_count, (at + 3) * row_count)
            real = even[one] * tw(0) + odd[one] * tw(2) + even[two] * tw(4) + odd[two] * tw(6)
            imag = even[one] * tw(1) + odd[one] * tw(3) + even[two] * tw(5) + odd[two] * tw(7)
            spectra.append(jnp.concatenate([real, imag], axis=0))
        mine = class_rows(classes, me[0], TILE)
        table = jnp.concatenate([small[:base, :base], mine[:, :base]], axis=0)
        pulled = nn(table, jnp.concatenate(spectra, axis=1))
        hats = nt(jnp.concatenate([pulled[:, :rows], pulled[:, rows:]], axis=0), row_table[...])
        top, bottom = small[base : base + 1, :rows], small[base + 1 : base + 2, :rows]
        skip = base + TILE
        both = jnp.concatenate(
            [
                hats[:row_count] * bottom - hats[row_count:base] * top,
                hats[skip : skip + row_count] * bottom - hats[skip + row_count : skip + base] * top,
            ],
            axis=0,
        )
        own_left, own_right = hats[base + 4 : base + 5], hats[skip + base + 4 : skip + base + 5]
        shifts = nn(both, weight[...])
        lefts, rights = small[base + TILE : base + TILE + 1, :cols], small[base + TILE + 1 : base + TILE + 2, :cols]
        loads[0].wait()
        jump = jumps_in[...] + lefts * shifts[:row_count] - rights * shifts[row_count:]
        ends = nn(mine[:, :row_count], systems[:row_count] * jump)
        number = row_number((TILE, rows))
        down = jnp.where(number == 2, own_left, jnp.where(number == 3, -own_right, small[base : base + TILE, rows : 2 * rows]))
        number = row_number((TILE, cols))
        along = jnp.where(number == 0, ends[5:6], jnp.where(number == 1, ends[6:7], small[base + 4 * TILE : base + 5 * TILE, :cols]))
        down = jnp.where(row_number(down.shape) < 4, down, 0.0)
        loads[1].wait()
        spectrum = weight[...] * (block_in[...] + outer(down, along))
        loads[2].wait()
        halfway = three(spectrum, col_in[...], ((1,), (0,)))
        loads[3].wait()
        copies = []
        for at in range(2):
            span = slice(at * rows // 2, (at + 1) * rows // 2)
            ready[span] = three(row_table[:, span], halfway, ((0,), (0,))) + ratio * direction_in[span]
            copy = pltpu.make_async_copy(ready.at[span], out.at[span], left_core.at[at])
            copy.start()
            copies.append(copy)
        for copy in copies:
            copy.wait()

    return systems_kernel, classes_kernel, folds_kernel, finish_kernel


def f32(table):
    return jnp.asarray(np.asarray(table, np.float32))


def call(kernel, name, outs, scalars, arrays, flops, scratch=(), room=16 * 2**20):
    spaces = dict(vmem=pltpu.VMEM, hbm=pltpu.HBM, window=pltpu.VMEM, smem=pltpu.SMEM)

    def shape_of(shape, kind):
        made = dict(vmem=pltpu.VMEM, hbm=pltpu.HBM).get(kind, jax.ShapeDtypeStruct)
        return made(shape, jnp.float32)

    def placed(array, kind):
        return array if kind == "window" else pltpu.with_memory_space_constraint(array, spaces[kind])

    moved = sum(4 * int(np.prod(shape)) for shape, _ in outs) + sum(4 * a.size for a, _ in arrays)
    return pl.pallas_call(
        kernel,
        out_shape=[shape_of(*entry) for entry in outs],
        in_specs=[pl.BlockSpec(memory_space=pltpu.SMEM)] * len(scalars)
        + [pl.BlockSpec(memory_space=spaces[kind]) for _, kind in arrays],
        out_specs=[pl.BlockSpec(memory_space=spaces[kind]) for _, kind in outs],
        scratch_shapes=list(scratch),
        name=name,
        compiler_params=pltpu.CompilerParams(vmem_limit_bytes=room),
        cost_estimate=pl.CostEstimate(flops=flops, bytes_accessed=moved, transcendentals=0),
    )(*scalars, *[placed(*entry) for entry in arrays])


def exchange(copies, axis):
    seen = lax.all_to_all(copies, axis, 0, 0, tiled=True)
    return seen.reshape(seen.shape[0] * seen.shape[1], seen.shape[2])


def body(of, row_count, col_count, field, direction, ground, previous):
    rows, cols = field.shape
    half = rows // 2
    me_row = lax.axis_index(ROW).reshape(1)
    me_col = lax.axis_index(COL).reshape(1)
    k = {name: f32(table) for name, table in of.items()}
    systems_kernel, classes_kernel, folds_kernel, finish_kernel = make_kernels(row_count, col_count, rows, cols)

    def space(shape):
        return pltpu.VMEM(shape, jnp.float32)

    two = pltpu.SemaphoreType.DMA((2,))

    def hold(*arrays):
        return [(array, "vmem") for array in arrays]

    loads = (field, k["col_table"], k["row_table"], k["columns"], k["sends"])
    block, weight, send = call(
        edges_kernel,
        "edges",
        [((rows, cols), "hbm"), ((rows, cols), "vmem"), ((row_count // 2, 2 * TILE, half), "hbm")],
        [ground],
        [(array, "hbm") for array in loads],
        2 * rows * cols * (rows + cols),
        [space(array.shape) for array in loads]
        + [pltpu.SemaphoreType.DMA((len(loads),)), space((rows, cols)), space((row_count // 2, 2 * TILE, half)), two],
    )
    seen = lax.all_gather(lax.all_to_all(send, PAIR, 0, 0, tiled=True), CORE)
    seen = seen.reshape(2 * TILE * row_count, half)
    (systems,) = call(
        systems_kernel,
        "systems",
        [((row_count + max(col_count, 2 * TILE), cols), "window")],
        [ground, me_row],
        hold(weight, k["columns"], k["small"], k["classes"]),
        2 * rows * cols * 32,
    )
    jumps, send = call(
        classes_kernel,
        "classes",
        [((row_count, cols), "hbm"), ((col_count, TILE, half), "hbm")],
        [me_row],
        hold(seen, weight, systems, k["row_table"], k["fine"], k["small"], k["classes"]),
        2 * rows * cols * 128,
        [space((row_count, cols)), space((col_count, TILE, half)), two],
    )
    seen = exchange(send, COL)
    (send,) = call(
        folds_kernel,
        "folds",
        [((row_count * WAVES, half), "hbm")],
        [me_col],
        hold(seen, systems, k["leaps"]),
        2 * rows * cols * 16,
        [space((row_count * WAVES, half)), two],
    )
    seen = exchange(send.reshape(row_count, 1, WAVES * half), ROW).reshape(row_count * WAVES, half)
    late = (jumps, block, k["col_table"], direction)
    out, ratio = call(
        finish_kernel,
        "finish",
        [((rows, cols), "hbm"), ((1,), "smem")],
        [previous, me_row],
        hold(seen, weight, systems, k["fine"], k["small"], k["classes"], k["row_table"])
        + [(array, "hbm") for array in late],
        2 * rows * cols * (rows + cols + 128),
        [space(array.shape) for array in late]
        + [pltpu.SemaphoreType.DMA((len(late),)), space((rows, cols)), pltpu.SemaphoreType.DMA((4,))],
    )
    return out, ratio


def solution(mesh):
    row_count, col_count = mesh.shape["row"], mesh.shape[COL]
    finer = Mesh(mesh.devices.reshape(row_count // 2, 2, col_count), (PAIR, CORE, COL))

    def step(residual, direction, ground_shift, previous):
        rows, cols = residual.shape[0] // row_count, residual.shape[1] // col_count
        of = kernel_constants(rows, cols, row_count, col_count)

        def local(field, heading, ground, last):
            return body(of, row_count, col_count, field, heading, ground, last)

        return jax.shard_map(
            local,
            mesh=finer,
            in_specs=(P(ROW, COL), P(ROW, COL), P(), P()),
            out_specs=(P(ROW, COL), P()),
            check_vma=False,
        )(residual, direction, ground_shift, previous)

    return step
```

```python
import numpy as np
import jax
import jax.numpy as jnp
from jax import lax
from jax.experimental import pallas as pl
from jax.experimental.pallas import tpu as pltpu
from jax.sharding import Mesh
from jax.sharding import PartitionSpec as P

ROW = ("pair", "core")
PAIR, CORE, COL = "pair", "core", "col"
TILE = 8
WAVES = 5
LANES = 128

HI = lax.Precision.HIGHEST


def cosines(length):
    wave = np.arange(length)[:, None]
    place = np.arange(length)[None, :]
    angle = np.pi * (wave * (2 * place + 1) % (4 * length)) / (2 * length)
    scale = np.where(wave == 0, np.sqrt(1.0 / length), np.sqrt(2.0 / length))
    return scale * np.cos(angle)


def stiffness(waves, length):
    return 4.0 * np.sin(np.pi * waves / (2 * length)) ** 2


def sines(blocks):
    index = np.arange(blocks + 1)
    table = np.sqrt(2.0 / blocks) * np.sin(np.pi * (index[:, None] * index[None, :] % (2 * blocks)) / blocks)
    table[blocks] = 0.0
    return table[:, :blocks]


def block_constants(extent, blocks):
    table = cosines(extent)
    edge = table[:, 0]
    sign = np.where(np.arange(extent) % 2 == 0, 1.0, -1.0)
    dst = sines(blocks)
    theta = np.cos(np.pi * np.arange(blocks) / blocks)
    return dict(
        table=table,
        lam=stiffness(np.arange(extent), extent),
        edges=np.stack([edge, edge * sign]),
        columns=np.stack([edge, edge * sign], axis=1),
        squares=np.stack([edge**2 * (1 + sign), edge**2 * (1 - sign)]),
        dst=dst[:blocks],
        after=dst[1:],
        gaps=np.stack([1 - theta, 1 + theta], axis=1),
    )


def wave_constants(extent, blocks):
    length = extent * blocks
    half = extent // 2
    kind = np.arange(blocks)
    block = np.arange(blocks)
    angle = np.pi * (kind[:, None] * block[None, :] % (2 * blocks)) / blocks
    parity = np.where(block % 2 == 0, 1.0, -1.0)
    mix = np.stack([np.cos(angle), np.where(kind[:, None] > 0, np.sin(angle), parity[None, :])], axis=1)
    first = kind
    second = np.where(kind == 0, blocks, 2 * blocks - kind)
    place = 2 * np.arange(extent) + 1
    phase_one = np.pi * (first[:, None] * place[None, :] % (4 * length)) / (2 * length)
    phase_two = np.pi * (second[:, None] * place[None, :] % (4 * length)) / (2 * length)
    inner = (kind > 0)[:, None] * 1.0
    twiddle = np.stack(
        [
            np.cos(phase_one),
            -inner * np.sin(phase_one),
            -np.sin(phase_one),
            -inner * np.cos(phase_one),
            inner * np.cos(phase_two),
            np.where(kind[:, None] > 0, np.sin(phase_two), np.cos(phase_two)),
            -inner * np.sin(phase_two),
            np.where(kind[:, None] > 0, np.cos(phase_two), -np.sin(phase_two)),
        ],
        axis=1,
    )
    twiddle[0, 2] = 0.0
    steps = np.arange(half)
    fine = np.pi * (steps[None, :] * place[:, None] % (2 * extent)) / extent
    waves = np.stack([first, second], axis=1)[:, :, None] + 2 * blocks * steps[None, None, :]
    energy = np.where(waves == 0, 1.0 / length, 2.0 / length)
    return dict(
        mix=mix,
        twiddle=twiddle,
        fine=np.concatenate([np.cos(fine), np.sin(fine)], axis=0),
        lam=stiffness(waves, length),
        energy=energy,
    )


def kernel_constants(rows, cols, row_count, col_count):
    row = block_constants(rows, row_count)
    col = block_constants(cols, col_count)
    wave = wave_constants(rows, row_count)
    half = rows // 2
    top, bottom = row["edges"]
    left, right = col["edges"]
    mix, dst, after = wave["mix"], row["dst"], row["after"]
    dst_c, after_c = col["dst"], col["after"]
    unmix = np.concatenate([mix[:, 0].T, mix[:, 1].T], axis=1)

    order = np.concatenate([np.arange(0, row_count, 2), np.arange(1, row_count, 2)])
    columns = np.zeros((rows, LANES))
    columns[:, 0] = row["lam"]
    columns[:, 5] = top
    for piece in range(cols // rows):
        columns[:, 8 + piece] = col["lam"][piece * rows : (piece + 1) * rows]
    columns[:row_count, 1:3] = row["gaps"]
    columns[:col_count, 3:5] = col["gaps"]

    sends = np.zeros((3 * TILE, cols))
    group = min(LANES, cols)
    sends[4, :group] = 1.0
    sends[5, :group] = np.where(np.arange(group) % 2 == 0, 1.0, -1.0)
    sends[2 * TILE + 1] = left
    sends[2 * TILE] = col["lam"]

    small = np.zeros((2 * row_count + 5 * TILE, max(3 * LANES, 2 * rows, cols)))
    small[: 2 * row_count, : 2 * row_count] = np.concatenate([after.T @ unmix, dst.T @ unmix], axis=0)
    small[:row_count, LANES : LANES + 2 * row_count] = np.concatenate([after.T[:, order], -dst.T[:, order]], axis=1)
    small[:row_count, 2 * LANES : 2 * LANES + row_count] = dst
    small[row_count : 2 * row_count, 2 * LANES : 2 * LANES + row_count] = after
    base = 2 * row_count
    small[base, :rows], small[base + 1, :rows] = top, bottom
    small[base, rows : 2 * rows], small[base + 1, rows : 2 * rows] = top, -bottom
    small[base + TILE, :cols], small[base + TILE + 1, :cols] = left, right
    small[base + 2 * TILE : base + 2 * TILE + 2, :rows] = row["squares"]
    small[base + 3 * TILE : base + 3 * TILE + 2, :cols] = col["squares"]
    small[base + 4 * TILE + 2, :cols], small[base + 4 * TILE + 3, :cols] = left, right

    leaps = np.zeros((2 * col_count + TILE, TILE * col_count))
    reach = max(LANES, TILE * col_count)
    leaps[:col_count, 1::TILE], leaps[:col_count, 0::TILE] = after_c.T, -dst_c.T
    leaps[col_count : 2 * col_count, 3::TILE], leaps[col_count : 2 * col_count, 2::TILE] = after_c.T, -dst_c.T
    leaps[2 * col_count, 4::TILE] = 1.0
    own_c = np.zeros((TILE * col_count, col_count))
    for at in (0, 2):
        own_c[at::TILE], own_c[at + 1 :: TILE] = dst_c, after_c

    classes = np.zeros((row_count, 2 * TILE, max(rows, 2 * row_count)))
    classes[:, :TILE, :rows] = wave["twiddle"]
    classes[:, 8, :rows] = wave["lam"].reshape(row_count, rows)
    classes[:, 9, :rows] = wave["energy"].reshape(row_count, rows)
    classes[:, 10, :row_count], classes[:, 11, :row_count] = mix[:, 0], mix[:, 1]
    classes[:, 10, half : half + row_count], classes[:, 11, half : half + row_count] = mix[:, 0][:, order], mix[:, 1][:, order]
    classes[:, 12, : 2 * row_count] = unmix
    classes[:, 13, :row_count], classes[:, 14, :row_count] = dst, after
    slabs = [classes[:, :, :half], classes[:, :, half:rows]]
    return dict(
        row_table=row["table"],
        col_table=col["table"],
        columns=columns,
        sends=sends,
        small=small,
        leaps=np.concatenate(
            [np.pad(table, ((0, 0), (0, reach - table.shape[1]))) for table in (own_c, leaps)], axis=0
        ),
        classes=np.concatenate([slab.reshape(2 * TILE * row_count, half) for slab in slabs], axis=0),
        fine=wave["fine"],
    )


def nn(a, b):
    return lax.dot_general(a, b, (((1,), (0,)), ((), ())), precision=HI, preferred_element_type=jnp.float32)


def nt(a, b):
    return lax.dot_general(a, b, (((1,), (1,)), ((), ())), precision=HI, preferred_element_type=jnp.float32)


def halves(a):
    high = a.astype(jnp.bfloat16)
    return high, (a - high.astype(jnp.float32)).astype(jnp.bfloat16)


def three(a, b, dims):
    def dot(x, y):
        return lax.dot_general(x, y, (dims, ((), ())), preferred_element_type=jnp.float32)

    (a_high, a_low), (b_high, b_low) = halves(a), halves(b)
    return dot(a_high, b_high) + (dot(a_high, b_low) + dot(a_low, b_high))


def thirds(a):
    high = a.astype(jnp.bfloat16).astype(jnp.float32)
    rest = a - high
    middle = rest.astype(jnp.bfloat16).astype(jnp.float32)
    return high, middle, rest - middle


def outer(a, b):
    (a_one, a_two, a_three), (b_one, b_two, b_three) = thirds(a), thirds(b)
    left = jnp.concatenate([a_one, a_one, a_two, a_one, a_two, a_three], axis=0).astype(jnp.bfloat16)
    right = jnp.concatenate([b_one, b_two, b_one, b_three, b_two, b_one], axis=0).astype(jnp.bfloat16)
    return lax.dot_general(left, right, (((0,), (0,)), ((), ())), preferred_element_type=jnp.float32)


def row_number(shape):
    return lax.broadcasted_iota(jnp.int32, shape, 0)


def send_all(out_ref, copies_ref, sent, tile):
    for peer in range(out_ref.shape[0]):
        copies_ref[peer] = tile
    copy = pltpu.make_async_copy(copies_ref, out_ref, sent)
    copy.start()
    copy.wait()


def aligned(index, size):
    return pl.ds(pl.multiple_of(index * size, size), size)


def class_rows(classes, me, first):
    start = pl.multiple_of(me * 2 * TILE, TILE) + first
    slab = classes.shape[0] // 2
    return jnp.concatenate([classes[pl.ds(start, TILE), :], classes[pl.ds(slab + start, TILE), :]], axis=1)


def edges_kernel(g, field, col_table, row_table, columns, sends, block_out, weight_out, send_out, field_in, col_in, row_in, columns_in, sends_in, arrived, block_here, copies_here, left_core):
    rows, cols = field.shape
    pairs = [(row_table, row_in), (field, field_in), (columns, columns_in), (sends, sends_in), (col_table, col_in)]
    copies = [pltpu.make_async_copy(src, dst, arrived.at[at]) for at, (src, dst) in enumerate(pairs)]
    for copy in copies:
        copy.start()
    copies[0].wait()
    copies[1].wait()
    halfway = three(row_in[...], field_in[...], ((1,), (0,)))
    copies[2].wait()
    copies[3].wait()
    weight = 1.0 / (columns_in[:, 0:1] + sends_in[2 * TILE : 2 * TILE + 1] + g[0])
    weight_out[...] = weight
    copies[4].wait()
    block = three(halfway, col_in[...], ((1,), (1,)))
    solved = weight * block
    block_here[...] = block
    keep = pltpu.make_async_copy(block_here, block_out, left_core.at[0])
    keep.start()
    energy = jnp.sum(solved * block)
    number = row_number((TILE, rows))
    folded = jnp.sum((solved * columns_in[:, 5:6]).reshape(rows // TILE, TILE, cols), axis=0)
    tops = jnp.sum(folded, axis=0, keepdims=True)
    bottoms = jnp.sum(jnp.where(row_number(folded.shape) % 2 == 0, folded, -folded), axis=0, keepdims=True)
    sided = solved * sends_in[2 * TILE + 1 : 2 * TILE + 2]
    group = min(LANES, cols)
    sided = sum(sided[:, at : at + group] for at in range(0, cols, group))
    tile = nt(sends_in[:TILE, :group], sided)
    tile = jnp.where(number == 0, tops[:, :rows], jnp.where(number == 1, tops[:, rows:], tile))
    tile = jnp.where(number == 2, bottoms[:, :rows], jnp.where(number == 3, bottoms[:, rows:], tile))
    tile = jnp.where(row_number(tile.shape) == 6, energy, tile)
    tile = jnp.concatenate([tile[:, : rows // 2], tile[:, rows // 2 :]], axis=0)
    send_all(send_out, copies_here, left_core.at[1], tile)
    keep.wait()


def make_kernels(row_count, col_count, rows, cols):
    base = 2 * row_count
    half = rows // 2

    def systems_kernel(g, me, weight, columns, small, classes, out):
        sums = nn(small[base + 2 * TILE : base + 3 * TILE, :rows], weight[...])
        gaps = columns[:row_count, 1:3]
        out[:row_count] = 1.0 / (1.0 + gaps[:, 0:1] * sums[0:1] + gaps[:, 1:2] * sums[1:2])
        mine = class_rows(classes, me[0], TILE)
        down = jnp.concatenate([columns[:, 8 + piece : 9 + piece] for piece in range(cols // rows)], axis=0)
        long_weight = 1.0 / (down + mine[0:1] + g[0])
        sums = nn(small[base + 3 * TILE : base + 4 * TILE, :cols], long_weight)
        gaps = columns[:col_count, 3:5]
        out[row_count : row_count + col_count, :rows] = mine[1:2] / (1.0 + gaps[:, 0:1] * sums[0:1] + gaps[:, 1:2] * sums[1:2])
        sines_here = small[:base, 2 * LANES : 2 * LANES + row_count]
        out[row_count : row_count + TILE, rows : rows + row_count] = nn(mine[:, :row_count], sines_here[:row_count])
        out[row_count + TILE : row_count + 2 * TILE, rows : rows + row_count] = nn(mine[:, :row_count], sines_here[row_count:])

    def classes_kernel(me, seen, weight, systems, row_table, fine, small, classes, jumps_out, send_out, jumps_here, copies_here, left_core):
        def strided(at):
            parts = [seen[pl.ds(at + side, row_count, stride=2 * TILE), :] for side in (0, TILE)]
            return jnp.concatenate(parts, axis=1)

        lows = jnp.concatenate([strided(2), strided(0)], axis=0)
        highs = jnp.concatenate([strided(3), strided(1)], axis=0)
        jump_table = small[:row_count, LANES : LANES + 2 * row_count]
        jumps = nn(jump_table, jnp.concatenate([lows, highs], axis=1))
        jumps_here[...] = jumps
        keep = pltpu.make_async_copy(jumps_here, jumps_out, left_core.at[0])
        keep.start()
        bends = systems[:row_count] * jumps
        energy = jnp.sum(strided(6)[:, 0:1]) - jnp.sum(bends * jumps)
        lefts, rights = small[base + TILE : base + TILE + 1, :cols], small[base + TILE + 1 : base + TILE + 2, :cols]
        moved = nt(jnp.concatenate([bends * lefts, bends * rights], axis=0), weight[...])
        moved = jnp.concatenate([moved[:row_count], moved[row_count:]], axis=1)
        mine = class_rows(classes, me[0], TILE)[:, half : half + row_count]
        mixed = nn(mine, jnp.concatenate([strided(4), strided(5)], axis=1))
        top, bottom = small[base : base + 1, :rows], small[base + 1 : base + 2, :rows]
        bent = nn(systems[row_count : row_count + 2 * TILE, rows : rows + row_count], moved)
        mixed = (
            mixed
            + bent[:TILE] * jnp.concatenate([top, top], axis=1)
            - bent[TILE : 2 * TILE] * jnp.concatenate([bottom, bottom], axis=1)
        )
        placed = nn(jnp.concatenate([mixed[:, :rows], mixed[:, rows:]], axis=0), row_table[...])
        number = row_number((TILE, rows))
        lefty = lax.rem(number, 2) == 0
        real = jnp.where(lefty, placed[2:3], placed[TILE + 2 : TILE + 3])
        imag = jnp.where(lefty, placed[3:4], placed[TILE + 3 : TILE + 4])
        tw = class_rows(classes, me[0], 0)
        opening = number < 2
        even = real * jnp.where(opening, tw[0:1], tw[4:5]) + imag * jnp.where(opening, tw[1:2], tw[5:6])
        odd = real * jnp.where(opening, tw[2:3], tw[6:7]) + imag * jnp.where(opening, tw[3:4], tw[7:8])
        tile = three(jnp.concatenate([even, odd], axis=1), fine[...], ((1,), (0,)))
        send_all(send_out, copies_here, left_core.at[1], jnp.where(row_number(tile.shape) == 4, energy, tile))
        keep.wait()

    def folds_kernel(me, seen, systems, leaps, send_out, copies_here, left_core):
        skip = TILE * col_count
        out = nn(leaps[skip:, :skip], seen[...])
        first, second = out[:col_count], out[col_count : 2 * col_count]
        fold_first = systems[row_count : row_count + col_count, :half] * first
        fold_second = systems[row_count : row_count + col_count, half:rows] * second
        energy = out[2 * col_count : 2 * col_count + 1, 0:1] / row_count
        energy = energy - jnp.sum(fold_first * first + fold_second * second)
        table = leaps[aligned(me[0], TILE), :col_count]
        tile = jnp.where(row_number((TILE, half)) < 2, nn(table, fold_first), nn(table, fold_second))
        tile = jnp.where(row_number(tile.shape) == 4, energy, tile)
        for peer in range(row_count):
            copies_here[pl.ds(peer * WAVES, WAVES), :] = tile[:WAVES]
        copy = pltpu.make_async_copy(copies_here, send_out, left_core.at[0])
        copy.start()
        copy.wait()

    def finish_kernel(previous, me, seen, weight, systems, fine, small, classes, row_table, jumps, block, col_table, direction, out, ratio_out, jumps_in, block_in, col_in, direction_in, arrived, ready, left_core):
        pairs = [(jumps, jumps_in), (block, block_in), (col_table, col_in), (direction, direction_in)]
        loads = [pltpu.make_async_copy(src, dst, arrived.at[at]) for at, (src, dst) in enumerate(pairs)]
        for load in loads:
            load.start()

        def strided(at):
            return seen[pl.ds(at, row_count, stride=WAVES), :]

        def tw(at):
            slab = classes.shape[0] // 2
            parts = [classes[pl.ds(at + side, row_count, stride=2 * TILE), :] for side in (0, slab)]
            return jnp.concatenate(parts, axis=1)

        waves = jnp.concatenate([strided(0), strided(1), strided(2), strided(3)], axis=0)
        ratio = jnp.sum(strided(4)[:, 0:1]) / previous[0]
        ratio_out[0] = ratio
        both = three(waves, fine[...], ((1,), (1,)))
        even, odd = both[:, :rows], both[:, rows:]
        spectra = []
        for at in range(2):
            one, two = slice(at * row_count, (at + 1) * row_count), slice((at + 2) * row_count, (at + 3) * row_count)
            real = even[one] * tw(0) + odd[one] * tw(2) + even[two] * tw(4) + odd[two] * tw(6)
            imag = even[one] * tw(1) + odd[one] * tw(3) + even[two] * tw(5) + odd[two] * tw(7)
            spectra.append(jnp.concatenate([real, imag], axis=0))
        mine = class_rows(classes, me[0], TILE)
        table = jnp.concatenate([small[:base, :base], mine[:, :base]], axis=0)
        pulled = nn(table, jnp.concatenate(spectra, axis=1))
        hats = three(jnp.concatenate([pulled[:, :rows], pulled[:, rows:]], axis=0), row_table[...], ((1,), (1,)))
        top, bottom = small[base : base + 1, :rows], small[base + 1 : base + 2, :rows]
        skip = base + TILE
        both = jnp.concatenate(
            [
                hats[:row_count] * bottom - hats[row_count:base] * top,
                hats[skip : skip + row_count] * bottom - hats[skip + row_count : skip + base] * top,
            ],
            axis=0,
        )
        own_left, own_right = hats[base + 4 : base + 5], hats[skip + base + 4 : skip + base + 5]
        shifts = nn(both, weight[...])
        lefts, rights = small[base + TILE : base + TILE + 1, :cols], small[base + TILE + 1 : base + TILE + 2, :cols]
        loads[0].wait()
        jump = jumps_in[...] + lefts * shifts[:row_count] - rights * shifts[row_count:]
        ends = nn(mine[:, :row_count], systems[:row_count] * jump)
        number = row_number((TILE, rows))
        down = jnp.where(number == 2, own_left, jnp.where(number == 3, -own_right, small[base : base + TILE, rows : 2 * rows]))
        number = row_number((TILE, cols))
        along = jnp.where(number == 0, ends[5:6], jnp.where(number == 1, ends[6:7], small[base + 4 * TILE : base + 5 * TILE, :cols]))
        down = jnp.where(row_number(down.shape) < 4, down, 0.0)
        loads[1].wait()
        spectrum = weight[...] * (block_in[...] + outer(down, along))
        loads[2].wait()
        halfway = three(spectrum, col_in[...], ((1,), (0,)))
        loads[3].wait()
        copies = []
        for at in range(2):
            span = slice(at * rows // 2, (at + 1) * rows // 2)
            ready[span] = three(row_table[:, span], halfway, ((0,), (0,))) + ratio * direction_in[span]
            copy = pltpu.make_async_copy(ready.at[span], out.at[span], left_core.at[at])
            copy.start()
            copies.append(copy)
        for copy in copies:
            copy.wait()

    return systems_kernel, classes_kernel, folds_kernel, finish_kernel


def f32(table):
    return jnp.asarray(np.asarray(table, np.float32))


def call(kernel, name, outs, scalars, arrays, flops, scratch=(), room=16 * 2**20):
    spaces = dict(vmem=pltpu.VMEM, hbm=pltpu.HBM, window=pltpu.VMEM, smem=pltpu.SMEM)

    def shape_of(shape, kind):
        made = dict(vmem=pltpu.VMEM, hbm=pltpu.HBM).get(kind, jax.ShapeDtypeStruct)
        return made(shape, jnp.float32)

    def placed(array, kind):
        return array if kind == "window" else pltpu.with_memory_space_constraint(array, spaces[kind])

    moved = sum(4 * int(np.prod(shape)) for shape, _ in outs) + sum(4 * a.size for a, _ in arrays)
    return pl.pallas_call(
        kernel,
        out_shape=[shape_of(*entry) for entry in outs],
        in_specs=[pl.BlockSpec(memory_space=pltpu.SMEM)] * len(scalars)
        + [pl.BlockSpec(memory_space=spaces[kind]) for _, kind in arrays],
        out_specs=[pl.BlockSpec(memory_space=spaces[kind]) for _, kind in outs],
        scratch_shapes=list(scratch),
        name=name,
        compiler_params=pltpu.CompilerParams(vmem_limit_bytes=room),
        cost_estimate=pl.CostEstimate(flops=flops, bytes_accessed=moved, transcendentals=0),
    )(*scalars, *[placed(*entry) for entry in arrays])


def exchange(copies, axis):
    seen = lax.all_to_all(copies, axis, 0, 0, tiled=True)
    return seen.reshape(seen.shape[0] * seen.shape[1], seen.shape[2])


def body(of, row_count, col_count, field, direction, ground, previous):
    rows, cols = field.shape
    half = rows // 2
    me_row = lax.axis_index(ROW).reshape(1)
    me_col = lax.axis_index(COL).reshape(1)
    k = {name: f32(table) for name, table in of.items()}
    systems_kernel, classes_kernel, folds_kernel, finish_kernel = make_kernels(row_count, col_count, rows, cols)

    def space(shape):
        return pltpu.VMEM(shape, jnp.float32)

    two = pltpu.SemaphoreType.DMA((2,))

    def hold(*arrays):
        return [(array, "vmem") for array in arrays]

    loads = (field, k["col_table"], k["row_table"], k["columns"], k["sends"])
    block, weight, send = call(
        edges_kernel,
        "edges",
        [((rows, cols), "hbm"), ((rows, cols), "vmem"), ((row_count // 2, 2 * TILE, half), "hbm")],
        [ground],
        [(array, "hbm") for array in loads],
        2 * rows * cols * (rows + cols),
        [space(array.shape) for array in loads]
        + [pltpu.SemaphoreType.DMA((len(loads),)), space((rows, cols)), space((row_count // 2, 2 * TILE, half)), two],
    )
    seen = lax.all_gather(lax.all_to_all(send, PAIR, 0, 0, tiled=True), CORE)
    seen = seen.reshape(2 * TILE * row_count, half)
    (systems,) = call(
        systems_kernel,
        "systems",
        [((row_count + max(col_count, 2 * TILE), cols), "window")],
        [ground, me_row],
        hold(weight, k["columns"], k["small"], k["classes"]),
        2 * rows * cols * 32,
    )
    jumps, send = call(
        classes_kernel,
        "classes",
        [((row_count, cols), "hbm"), ((col_count, TILE, half), "hbm")],
        [me_row],
        hold(seen, weight, systems, k["row_table"], k["fine"], k["small"], k["classes"]),
        2 * rows * cols * 128,
        [space((row_count, cols)), space((col_count, TILE, half)), two],
    )
    seen = exchange(send, COL)
    (send,) = call(
        folds_kernel,
        "folds",
        [((row_count * WAVES, half), "hbm")],
        [me_col],
        hold(seen, systems, k["leaps"]),
        2 * rows * cols * 16,
        [space((row_count * WAVES, half)), two],
    )
    seen = exchange(send.reshape(row_count, 1, WAVES * half), ROW).reshape(row_count * WAVES, half)
    late = (jumps, block, k["col_table"], direction)
    out, ratio = call(
        finish_kernel,
        "finish",
        [((rows, cols), "hbm"), ((1,), "smem")],
        [previous, me_row],
        hold(seen, weight, systems, k["fine"], k["small"], k["classes"], k["row_table"])
        + [(array, "hbm") for array in late],
        2 * rows * cols * (rows + cols + 128),
        [space(array.shape) for array in late]
        + [pltpu.SemaphoreType.DMA((len(late),)), space((rows, cols)), pltpu.SemaphoreType.DMA((4,))],
    )
    return out, ratio


def solution(mesh):
    row_count, col_count = mesh.shape["row"], mesh.shape[COL]
    finer = Mesh(mesh.devices.reshape(row_count // 2, 2, col_count), (PAIR, CORE, COL))

    def step(residual, direction, ground_shift, previous):
        rows, cols = residual.shape[0] // row_count, residual.shape[1] // col_count
        of = kernel_constants(rows, cols, row_count, col_count)

        def local(field, heading, ground, last):
            return body(of, row_count, col_count, field, heading, ground, last)

        return jax.shard_map(
            local,
            mesh=finer,
            in_specs=(P(ROW, COL), P(ROW, COL), P(), P()),
            out_specs=(P(ROW, COL), P()),
            check_vma=False,
        )(residual, direction, ground_shift, previous)

    return step
```

```python
import numpy as np
import jax
import jax.numpy as jnp
from jax import lax
from jax.experimental import pallas as pl
from jax.experimental.pallas import tpu as pltpu
from jax.sharding import Mesh
from jax.sharding import PartitionSpec as P

ROW = ("pair", "core")
PAIR, CORE, COL = "pair", "core", "col"
TILE = 8
WAVES = 5
LANES = 128

HI = lax.Precision.HIGHEST


def cosines(length):
    wave = np.arange(length)[:, None]
    place = np.arange(length)[None, :]
    angle = np.pi * (wave * (2 * place + 1) % (4 * length)) / (2 * length)
    scale = np.where(wave == 0, np.sqrt(1.0 / length), np.sqrt(2.0 / length))
    return scale * np.cos(angle)


def stiffness(waves, length):
    return 4.0 * np.sin(np.pi * waves / (2 * length)) ** 2


def sines(blocks):
    index = np.arange(blocks + 1)
    table = np.sqrt(2.0 / blocks) * np.sin(np.pi * (index[:, None] * index[None, :] % (2 * blocks)) / blocks)
    table[blocks] = 0.0
    return table[:, :blocks]


def block_constants(extent, blocks):
    table = cosines(extent)
    edge = table[:, 0]
    sign = np.where(np.arange(extent) % 2 == 0, 1.0, -1.0)
    dst = sines(blocks)
    theta = np.cos(np.pi * np.arange(blocks) / blocks)
    return dict(
        table=table,
        lam=stiffness(np.arange(extent), extent),
        edges=np.stack([edge, edge * sign]),
        columns=np.stack([edge, edge * sign], axis=1),
        squares=np.stack([edge**2 * (1 + sign), edge**2 * (1 - sign)]),
        dst=dst[:blocks],
        after=dst[1:],
        gaps=np.stack([1 - theta, 1 + theta], axis=1),
    )


def wave_constants(extent, blocks):
    length = extent * blocks
    half = extent // 2
    kind = np.arange(blocks)
    block = np.arange(blocks)
    angle = np.pi * (kind[:, None] * block[None, :] % (2 * blocks)) / blocks
    parity = np.where(block % 2 == 0, 1.0, -1.0)
    mix = np.stack([np.cos(angle), np.where(kind[:, None] > 0, np.sin(angle), parity[None, :])], axis=1)
    first = kind
    second = np.where(kind == 0, blocks, 2 * blocks - kind)
    place = 2 * np.arange(extent) + 1
    phase_one = np.pi * (first[:, None] * place[None, :] % (4 * length)) / (2 * length)
    phase_two = np.pi * (second[:, None] * place[None, :] % (4 * length)) / (2 * length)
    inner = (kind > 0)[:, None] * 1.0
    twiddle = np.stack(
        [
            np.cos(phase_one),
            -inner * np.sin(phase_one),
            -np.sin(phase_one),
            -inner * np.cos(phase_one),
            inner * np.cos(phase_two),
            np.where(kind[:, None] > 0, np.sin(phase_two), np.cos(phase_two)),
            -inner * np.sin(phase_two),
            np.where(kind[:, None] > 0, np.cos(phase_two), -np.sin(phase_two)),
        ],
        axis=1,
    )
    twiddle[0, 2] = 0.0
    steps = np.arange(half)
    fine = np.pi * (steps[None, :] * place[:, None] % (2 * extent)) / extent
    waves = np.stack([first, second], axis=1)[:, :, None] + 2 * blocks * steps[None, None, :]
    energy = np.where(waves == 0, 1.0 / length, 2.0 / length)
    return dict(
        mix=mix,
        twiddle=twiddle,
        fine=np.concatenate([np.cos(fine), np.sin(fine)], axis=0),
        lam=stiffness(waves, length),
        energy=energy,
    )


def kernel_constants(rows, cols, row_count, col_count):
    row = block_constants(rows, row_count)
    col = block_constants(cols, col_count)
    wave = wave_constants(rows, row_count)
    half = rows // 2
    top, bottom = row["edges"]
    left, right = col["edges"]
    mix, dst, after = wave["mix"], row["dst"], row["after"]
    dst_c, after_c = col["dst"], col["after"]
    unmix = np.concatenate([mix[:, 0].T, mix[:, 1].T], axis=1)

    order = np.concatenate([np.arange(0, row_count, 2), np.arange(1, row_count, 2)])
    columns = np.zeros((rows, LANES))
    columns[:, 0] = row["lam"]
    columns[:, 5] = top
    for piece in range(cols // rows):
        columns[:, 8 + piece] = col["lam"][piece * rows : (piece + 1) * rows]
    columns[:row_count, 1:3] = row["gaps"]
    columns[:col_count, 3:5] = col["gaps"]

    sends = np.zeros((3 * TILE, cols))
    group = min(LANES, cols)
    sends[4, :group] = 1.0
    sends[5, :group] = np.where(np.arange(group) % 2 == 0, 1.0, -1.0)
    sends[2 * TILE + 1] = left
    sends[2 * TILE] = col["lam"]

    small = np.zeros((2 * row_count + 5 * TILE, max(3 * LANES, 2 * rows, cols)))
    small[: 2 * row_count, : 2 * row_count] = np.concatenate([after.T @ unmix, dst.T @ unmix], axis=0)
    small[:row_count, LANES : LANES + 2 * row_count] = np.concatenate([after.T[:, order], -dst.T[:, order]], axis=1)
    small[:row_count, 2 * LANES : 2 * LANES + row_count] = dst
    small[row_count : 2 * row_count, 2 * LANES : 2 * LANES + row_count] = after
    base = 2 * row_count
    small[base, :rows], small[base + 1, :rows] = top, bottom
    small[base, rows : 2 * rows], small[base + 1, rows : 2 * rows] = top, -bottom
    small[base + TILE, :cols], small[base + TILE + 1, :cols] = left, right
    small[base + 2 * TILE : base + 2 * TILE + 2, :rows] = row["squares"]
    small[base + 3 * TILE : base + 3 * TILE + 2, :cols] = col["squares"]
    small[base + 4 * TILE + 2, :cols], small[base + 4 * TILE + 3, :cols] = left, right

    leaps = np.zeros((2 * col_count + TILE, TILE * col_count))
    reach = max(LANES, TILE * col_count)
    leaps[:col_count, 1::TILE], leaps[:col_count, 0::TILE] = after_c.T, -dst_c.T
    leaps[col_count : 2 * col_count, 3::TILE], leaps[col_count : 2 * col_count, 2::TILE] = after_c.T, -dst_c.T
    leaps[2 * col_count, 4::TILE] = 1.0
    own_c = np.zeros((TILE * col_count, col_count))
    for at in (0, 2):
        own_c[at::TILE], own_c[at + 1 :: TILE] = dst_c, after_c

    classes = np.zeros((row_count, 2 * TILE, max(rows, 2 * row_count)))
    classes[:, :TILE, :rows] = wave["twiddle"]
    classes[:, 8, :rows] = wave["lam"].reshape(row_count, rows)
    classes[:, 9, :rows] = wave["energy"].reshape(row_count, rows)
    classes[:, 10, :row_count], classes[:, 11, :row_count] = mix[:, 0], mix[:, 1]
    classes[:, 10, half : half + row_count], classes[:, 11, half : half + row_count] = mix[:, 0][:, order], mix[:, 1][:, order]
    classes[:, 12, : 2 * row_count] = unmix
    classes[:, 13, :row_count], classes[:, 14, :row_count] = dst, after
    slabs = [classes[:, :, :half], classes[:, :, half:rows]]
    return dict(
        row_table=row["table"],
        col_table=col["table"],
        columns=columns,
        sends=sends,
        small=small,
        leaps=np.concatenate(
            [np.pad(table, ((0, 0), (0, reach - table.shape[1]))) for table in (own_c, leaps)], axis=0
        ),
        classes=np.concatenate([slab.reshape(2 * TILE * row_count, half) for slab in slabs], axis=0),
        fine=wave["fine"],
    )


def nn(a, b):
    return lax.dot_general(a, b, (((1,), (0,)), ((), ())), precision=HI, preferred_element_type=jnp.float32)


def nt(a, b):
    return lax.dot_general(a, b, (((1,), (1,)), ((), ())), precision=HI, preferred_element_type=jnp.float32)


def halves(a):
    high = a.astype(jnp.bfloat16)
    return high, (a - high.astype(jnp.float32)).astype(jnp.bfloat16)


def three(a, b, dims):
    def dot(x, y):
        return lax.dot_general(x, y, (dims, ((), ())), preferred_element_type=jnp.float32)

    (a_high, a_low), (b_high, b_low) = halves(a), halves(b)
    return dot(a_high, b_high) + (dot(a_high, b_low) + dot(a_low, b_high))


def thirds(a):
    high = a.astype(jnp.bfloat16).astype(jnp.float32)
    rest = a - high
    middle = rest.astype(jnp.bfloat16).astype(jnp.float32)
    return high, middle, rest - middle


def outer(a, b):
    (a_one, a_two, a_three), (b_one, b_two, b_three) = thirds(a), thirds(b)
    left = jnp.concatenate([a_one, a_one, a_two, a_one, a_two, a_three], axis=0).astype(jnp.bfloat16)
    right = jnp.concatenate([b_one, b_two, b_one, b_three, b_two, b_one], axis=0).astype(jnp.bfloat16)
    return lax.dot_general(left, right, (((0,), (0,)), ((), ())), preferred_element_type=jnp.float32)


def row_number(shape):
    return lax.broadcasted_iota(jnp.int32, shape, 0)


def send_all(out_ref, copies_ref, sent, tile):
    for peer in range(out_ref.shape[0]):
        copies_ref[peer] = tile
    copy = pltpu.make_async_copy(copies_ref, out_ref, sent)
    copy.start()
    copy.wait()


def aligned(index, size):
    return pl.ds(pl.multiple_of(index * size, size), size)


def class_rows(classes, me, first):
    start = pl.multiple_of(me * 2 * TILE, TILE) + first
    slab = classes.shape[0] // 2
    return jnp.concatenate([classes[pl.ds(start, TILE), :], classes[pl.ds(slab + start, TILE), :]], axis=1)


def edges_kernel(g, field, col_table, row_table, columns, sends, block_out, weight_out, send_out, field_in, col_in, row_in, columns_in, sends_in, arrived, block_here, copies_here, left_core):
    rows, cols = field.shape
    pairs = [(row_table, row_in), (field, field_in), (columns, columns_in), (sends, sends_in), (col_table, col_in)]
    copies = [pltpu.make_async_copy(src, dst, arrived.at[at]) for at, (src, dst) in enumerate(pairs)]
    for copy in copies:
        copy.start()
    copies[0].wait()
    copies[1].wait()
    halfway = three(row_in[...], field_in[...], ((1,), (0,)))
    copies[2].wait()
    copies[3].wait()
    weight = 1.0 / (columns_in[:, 0:1] + sends_in[2 * TILE : 2 * TILE + 1] + g[0])
    weight_out[...] = weight
    copies[4].wait()
    block = three(halfway, col_in[...], ((1,), (1,)))
    solved = weight * block
    block_here[...] = block
    keep = pltpu.make_async_copy(block_here, block_out, left_core.at[0])
    keep.start()
    energy = jnp.sum(solved * block)
    number = row_number((TILE, rows))
    folded = jnp.sum((solved * columns_in[:, 5:6]).reshape(rows // TILE, TILE, cols), axis=0)
    tops = jnp.sum(folded, axis=0, keepdims=True)
    bottoms = jnp.sum(jnp.where(row_number(folded.shape) % 2 == 0, folded, -folded), axis=0, keepdims=True)
    sided = solved * sends_in[2 * TILE + 1 : 2 * TILE + 2]
    group = min(LANES, cols)
    sided = sum(sided[:, at : at + group] for at in range(0, cols, group))
    tile = nt(sends_in[:TILE, :group], sided)
    tile = jnp.where(number == 0, tops[:, :rows], jnp.where(number == 1, tops[:, rows:], tile))
    tile = jnp.where(number == 2, bottoms[:, :rows], jnp.where(number == 3, bottoms[:, rows:], tile))
    tile = jnp.where(row_number(tile.shape) == 6, energy, tile)
    tile = jnp.concatenate([tile[:, : rows // 2], tile[:, rows // 2 :]], axis=0)
    send_all(send_out, copies_here, left_core.at[1], tile)
    keep.wait()


def make_kernels(row_count, col_count, rows, cols):
    base = 2 * row_count
    half = rows // 2

    def systems_kernel(g, me, weight, columns, small, classes, out):
        sums = nn(small[base + 2 * TILE : base + 3 * TILE, :rows], weight[...])
        gaps = columns[:row_count, 1:3]
        out[:row_count] = 1.0 / (1.0 + gaps[:, 0:1] * sums[0:1] + gaps[:, 1:2] * sums[1:2])
        mine = class_rows(classes, me[0], TILE)
        down = jnp.concatenate([columns[:, 8 + piece : 9 + piece] for piece in range(cols // rows)], axis=0)
        long_weight = 1.0 / (down + mine[0:1] + g[0])
        sums = nn(small[base + 3 * TILE : base + 4 * TILE, :cols], long_weight)
        gaps = columns[:col_count, 3:5]
        out[row_count : row_count + col_count, :rows] = mine[1:2] / (1.0 + gaps[:, 0:1] * sums[0:1] + gaps[:, 1:2] * sums[1:2])
        sines_here = small[:base, 2 * LANES : 2 * LANES + row_count]
        out[row_count : row_count + TILE, rows : rows + row_count] = nn(mine[:, :row_count], sines_here[:row_count])
        out[row_count + TILE : row_count + 2 * TILE, rows : rows + row_count] = nn(mine[:, :row_count], sines_here[row_count:])

    def classes_kernel(me, seen, weight, systems, row_table, fine, small, classes, jumps_out, send_out, jumps_here, copies_here, left_core):
        def strided(at):
            parts = [seen[pl.ds(at + side, row_count, stride=2 * TILE), :] for side in (0, TILE)]
            return jnp.concatenate(parts, axis=1)

        lows = jnp.concatenate([strided(2), strided(0)], axis=0)
        highs = jnp.concatenate([strided(3), strided(1)], axis=0)
        jump_table = small[:row_count, LANES : LANES + 2 * row_count]
        jumps = nn(jump_table, jnp.concatenate([lows, highs], axis=1))
        jumps_here[...] = jumps
        keep = pltpu.make_async_copy(jumps_here, jumps_out, left_core.at[0])
        keep.start()
        bends = systems[:row_count] * jumps
        energy = jnp.sum(strided(6)[:, 0:1]) - jnp.sum(bends * jumps)
        lefts, rights = small[base + TILE : base + TILE + 1, :cols], small[base + TILE + 1 : base + TILE + 2, :cols]
        moved = nt(jnp.concatenate([bends * lefts, bends * rights], axis=0), weight[...])
        moved = jnp.concatenate([moved[:row_count], moved[row_count:]], axis=1)
        mine = class_rows(classes, me[0], TILE)[:, half : half + row_count]
        mixed = nn(mine, jnp.concatenate([strided(4), strided(5)], axis=1))
        top, bottom = small[base : base + 1, :rows], small[base + 1 : base + 2, :rows]
        bent = nn(systems[row_count : row_count + 2 * TILE, rows : rows + row_count], moved)
        mixed = (
            mixed
            + bent[:TILE] * jnp.concatenate([top, top], axis=1)
            - bent[TILE : 2 * TILE] * jnp.concatenate([bottom, bottom], axis=1)
        )
        placed = three(jnp.concatenate([mixed[:, :rows], mixed[:, rows:]], axis=0), row_table[...], ((1,), (0,)))
        number = row_number((TILE, rows))
        lefty = lax.rem(number, 2) == 0
        real = jnp.where(lefty, placed[2:3], placed[TILE + 2 : TILE + 3])
        imag = jnp.where(lefty, placed[3:4], placed[TILE + 3 : TILE + 4])
        tw = class_rows(classes, me[0], 0)
        opening = number < 2
        even = real * jnp.where(opening, tw[0:1], tw[4:5]) + imag * jnp.where(opening, tw[1:2], tw[5:6])
        odd = real * jnp.where(opening, tw[2:3], tw[6:7]) + imag * jnp.where(opening, tw[3:4], tw[7:8])
        tile = three(jnp.concatenate([even, odd], axis=1), fine[...], ((1,), (0,)))
        send_all(send_out, copies_here, left_core.at[1], jnp.where(row_number(tile.shape) == 4, energy, tile))
        keep.wait()

    def folds_kernel(me, seen, systems, leaps, send_out, copies_here, left_core):
        skip = TILE * col_count
        out = nn(leaps[skip:, :skip], seen[...])
        first, second = out[:col_count], out[col_count : 2 * col_count]
        fold_first = systems[row_count : row_count + col_count, :half] * first
        fold_second = systems[row_count : row_count + col_count, half:rows] * second
        energy = out[2 * col_count : 2 * col_count + 1, 0:1] / row_count
        energy = energy - jnp.sum(fold_first * first + fold_second * second)
        table = leaps[aligned(me[0], TILE), :col_count]
        tile = jnp.where(row_number((TILE, half)) < 2, nn(table, fold_first), nn(table, fold_second))
        tile = jnp.where(row_number(tile.shape) == 4, energy, tile)
        for peer in range(row_count):
            copies_here[pl.ds(peer * WAVES, WAVES), :] = tile[:WAVES]
        copy = pltpu.make_async_copy(copies_here, send_out, left_core.at[0])
        copy.start()
        copy.wait()

    def finish_kernel(previous, me, seen, weight, systems, fine, small, classes, row_table, jumps, block, col_table, direction, out, ratio_out, jumps_in, block_in, col_in, direction_in, arrived, ready, left_core):
        pairs = [(jumps, jumps_in), (block, block_in), (col_table, col_in), (direction, direction_in)]
        loads = [pltpu.make_async_copy(src, dst, arrived.at[at]) for at, (src, dst) in enumerate(pairs)]
        for load in loads:
            load.start()

        def strided(at):
            return seen[pl.ds(at, row_count, stride=WAVES), :]

        def tw(at):
            slab = classes.shape[0] // 2
            parts = [classes[pl.ds(at + side, row_count, stride=2 * TILE), :] for side in (0, slab)]
            return jnp.concatenate(parts, axis=1)

        waves = jnp.concatenate([strided(0), strided(1), strided(2), strided(3)], axis=0)
        ratio = jnp.sum(strided(4)[:, 0:1]) / previous[0]
        ratio_out[0] = ratio
        both = three(waves, fine[...], ((1,), (1,)))
        even, odd = both[:, :rows], both[:, rows:]
        spectra = []
        for at in range(2):
            one, two = slice(at * row_count, (at + 1) * row_count), slice((at + 2) * row_count, (at + 3) * row_count)
            real = even[one] * tw(0) + odd[one] * tw(2) + even[two] * tw(4) + odd[two] * tw(6)
            imag = even[one] * tw(1) + odd[one] * tw(3) + even[two] * tw(5) + odd[two] * tw(7)
            spectra.append(jnp.concatenate([real, imag], axis=0))
        mine = class_rows(classes, me[0], TILE)
        table = jnp.concatenate([small[:base, :base], mine[:, :base]], axis=0)
        pulled = nn(table, jnp.concatenate(spectra, axis=1))
        hats = three(jnp.concatenate([pulled[:, :rows], pulled[:, rows:]], axis=0), row_table[...], ((1,), (1,)))
        top, bottom = small[base : base + 1, :rows], small[base + 1 : base + 2, :rows]
        skip = base + TILE
        both = jnp.concatenate(
            [
                hats[:row_count] * bottom - hats[row_count:base] * top,
                hats[skip : skip + row_count] * bottom - hats[skip + row_count : skip + base] * top,
            ],
            axis=0,
        )
        own_left, own_right = hats[base + 4 : base + 5], hats[skip + base + 4 : skip + base + 5]
        shifts = nn(both, weight[...])
        lefts, rights = small[base + TILE : base + TILE + 1, :cols], small[base + TILE + 1 : base + TILE + 2, :cols]
        loads[0].wait()
        jump = jumps_in[...] + lefts * shifts[:row_count] - rights * shifts[row_count:]
        ends = nn(mine[:, :row_count], systems[:row_count] * jump)
        number = row_number((TILE, rows))
        down = jnp.where(number == 2, own_left, jnp.where(number == 3, -own_right, small[base : base + TILE, rows : 2 * rows]))
        number = row_number((TILE, cols))
        along = jnp.where(number == 0, ends[5:6], jnp.where(number == 1, ends[6:7], small[base + 4 * TILE : base + 5 * TILE, :cols]))
        down = jnp.where(row_number(down.shape) < 4, down, 0.0)
        loads[1].wait()
        spectrum = weight[...] * (block_in[...] + outer(down, along))
        loads[2].wait()
        halfway = three(spectrum, col_in[...], ((1,), (0,)))
        loads[3].wait()
        copies = []
        for at in range(2):
            span = slice(at * rows // 2, (at + 1) * rows // 2)
            ready[span] = three(row_table[:, span], halfway, ((0,), (0,))) + ratio * direction_in[span]
            copy = pltpu.make_async_copy(ready.at[span], out.at[span], left_core.at[at])
            copy.start()
            copies.append(copy)
        for copy in copies:
            copy.wait()

    return systems_kernel, classes_kernel, folds_kernel, finish_kernel


def f32(table):
    return jnp.asarray(np.asarray(table, np.float32))


def call(kernel, name, outs, scalars, arrays, flops, scratch=(), room=16 * 2**20):
    spaces = dict(vmem=pltpu.VMEM, hbm=pltpu.HBM, window=pltpu.VMEM, smem=pltpu.SMEM)

    def shape_of(shape, kind):
        made = dict(vmem=pltpu.VMEM, hbm=pltpu.HBM).get(kind, jax.ShapeDtypeStruct)
        return made(shape, jnp.float32)

    def placed(array, kind):
        return array if kind == "window" else pltpu.with_memory_space_constraint(array, spaces[kind])

    moved = sum(4 * int(np.prod(shape)) for shape, _ in outs) + sum(4 * a.size for a, _ in arrays)
    return pl.pallas_call(
        kernel,
        out_shape=[shape_of(*entry) for entry in outs],
        in_specs=[pl.BlockSpec(memory_space=pltpu.SMEM)] * len(scalars)
        + [pl.BlockSpec(memory_space=spaces[kind]) for _, kind in arrays],
        out_specs=[pl.BlockSpec(memory_space=spaces[kind]) for _, kind in outs],
        scratch_shapes=list(scratch),
        name=name,
        compiler_params=pltpu.CompilerParams(vmem_limit_bytes=room),
        cost_estimate=pl.CostEstimate(flops=flops, bytes_accessed=moved, transcendentals=0),
    )(*scalars, *[placed(*entry) for entry in arrays])


def exchange(copies, axis):
    seen = lax.all_to_all(copies, axis, 0, 0, tiled=True)
    return seen.reshape(seen.shape[0] * seen.shape[1], seen.shape[2])


def body(of, row_count, col_count, field, direction, ground, previous):
    rows, cols = field.shape
    half = rows // 2
    me_row = lax.axis_index(ROW).reshape(1)
    me_col = lax.axis_index(COL).reshape(1)
    k = {name: f32(table) for name, table in of.items()}
    systems_kernel, classes_kernel, folds_kernel, finish_kernel = make_kernels(row_count, col_count, rows, cols)

    def space(shape):
        return pltpu.VMEM(shape, jnp.float32)

    two = pltpu.SemaphoreType.DMA((2,))

    def hold(*arrays):
        return [(array, "vmem") for array in arrays]

    loads = (field, k["col_table"], k["row_table"], k["columns"], k["sends"])
    block, weight, send = call(
        edges_kernel,
        "edges",
        [((rows, cols), "hbm"), ((rows, cols), "vmem"), ((row_count // 2, 2 * TILE, half), "hbm")],
        [ground],
        [(array, "hbm") for array in loads],
        2 * rows * cols * (rows + cols),
        [space(array.shape) for array in loads]
        + [pltpu.SemaphoreType.DMA((len(loads),)), space((rows, cols)), space((row_count // 2, 2 * TILE, half)), two],
    )
    seen = lax.all_gather(lax.all_to_all(send, PAIR, 0, 0, tiled=True), CORE)
    seen = seen.reshape(2 * TILE * row_count, half)
    (systems,) = call(
        systems_kernel,
        "systems",
        [((row_count + max(col_count, 2 * TILE), cols), "window")],
        [ground, me_row],
        hold(weight, k["columns"], k["small"], k["classes"]),
        2 * rows * cols * 32,
    )
    jumps, send = call(
        classes_kernel,
        "classes",
        [((row_count, cols), "hbm"), ((col_count, TILE, half), "hbm")],
        [me_row],
        hold(seen, weight, systems, k["row_table"], k["fine"], k["small"], k["classes"]),
        2 * rows * cols * 128,
        [space((row_count, cols)), space((col_count, TILE, half)), two],
    )
    seen = exchange(send, COL)
    (send,) = call(
        folds_kernel,
        "folds",
        [((row_count * WAVES, half), "hbm")],
        [me_col],
        hold(seen, systems, k["leaps"]),
        2 * rows * cols * 16,
        [space((row_count * WAVES, half)), two],
    )
    seen = exchange(send.reshape(row_count, 1, WAVES * half), ROW).reshape(row_count * WAVES, half)
    late = (jumps, block, k["col_table"], direction)
    out, ratio = call(
        finish_kernel,
        "finish",
        [((rows, cols), "hbm"), ((1,), "smem")],
        [previous, me_row],
        hold(seen, weight, systems, k["fine"], k["small"], k["classes"], k["row_table"])
        + [(array, "hbm") for array in late],
        2 * rows * cols * (rows + cols + 128),
        [space(array.shape) for array in late]
        + [pltpu.SemaphoreType.DMA((len(late),)), space((rows, cols)), pltpu.SemaphoreType.DMA((4,))],
    )
    return out, ratio


def solution(mesh):
    row_count, col_count = mesh.shape["row"], mesh.shape[COL]
    finer = Mesh(mesh.devices.reshape(row_count // 2, 2, col_count), (PAIR, CORE, COL))

    def step(residual, direction, ground_shift, previous):
        rows, cols = residual.shape[0] // row_count, residual.shape[1] // col_count
        of = kernel_constants(rows, cols, row_count, col_count)

        def local(field, heading, ground, last):
            return body(of, row_count, col_count, field, heading, ground, last)

        return jax.shard_map(
            local,
            mesh=finer,
            in_specs=(P(ROW, COL), P(ROW, COL), P(), P()),
            out_specs=(P(ROW, COL), P()),
            check_vma=False,
        )(residual, direction, ground_shift, previous)

    return step
```
